128 devices in a mesh: dp: 16 (over y, x), expert: 4 (over z), tensor: 2 (over core).
Axes of the slice: x: 4, y: 4, z: 4, core: 2. Of those that a mesh axis runs over, the one named last changes fastest.
Arguments:
- tokens: bfloat16 [8192, 2048], P(('dp', 'expert'), 'tensor'), may hold values from -6 to 6
- norm_gain: bfloat16 [2048], replicated, may hold values from 0.25 to 1.75
- expert_ids: int32 [8192, 2], P(('dp', 'expert')), may hold values from 0 to 3, all different within a row; in each aligned block of 128 rows (0 to 127, 128 to 255, ...) at most 128 rows name the same one
- gate_codes: int32 [8192, 2], P(('dp', 'expert')), may hold values from 1 to 255
- gate_weights: bfloat16 [4, 7168, 2048], P('expert', ('dp', 'tensor')), may hold values from -0.125 to 0.125
- up_weights: bfloat16 [4, 7168, 2048], P('expert', ('dp', 'tensor')), may hold values from -0.125 to 0.125
- down_weights: bfloat16 [4, 7168, 2048], P('expert', ('dp', 'tensor')), may hold values from -0.0625 to 0.0625
- value_head: bfloat16 [2048, 128], replicated, may hold values from -0.125 to 0.125
- actions: int32 [8192], P(('dp', 'expert')), may hold values from 0 to 127
- rewards: int32 [8192], P(('dp', 'expert')), may hold values from -8 to 8
- trace_codes: int32 [8192], P(('dp', 'expert')), may hold values from 1 to 1024
Outputs:
- action_values: float32 [8192, 128], P(('dp', 'expert'))
- retrace_targets: float32 [8192], P(('dp', 'expert'))
The draws below stay inside these ranges and needn't reach their ends.
Inputs may be any that keep to these rules, and one draw needn't show every extreme that they name: `expert_ids`: each row names 2 different experts; within the 128 rows of one index pair of dp and expert each expert is named by at most 128 rows, and in some of these blocks one expert by exactly 128.
All inputs are finite; a program needn't handle non-finite values.
Results may differ from the reference program's by a relative error of at most 0.005.
Values may be sent and summed in bfloat16 or wider, within the bound.
A program may use at most 256 MiB of HBM per device.

```python
import math
import jax
import jax.numpy as jnp
import numpy as np
from jax import lax

D = 2048
FF = 7168
TOP = 2
NACT = 128
STEPS = 128
EXPERTS = 4
TOK_GRP = 128
CAP = 128
TOKENS = 8192


def draw_trace_codes(key, part):
    count = TOKENS // STEPS
    key_class = jax.random.fold_in(key, 11)
    key_plain = jax.random.fold_in(key, 12)
    key_where = jax.random.fold_in(key, 13)
    key_depth = jax.random.fold_in(key, 14)
    forgetful = jax.random.randint(key_class, (count, 1), 0, 4) == 0
    plain_codes = jax.random.randint(key_plain, (count, STEPS), 1, 1025)
    lowered = jax.random.randint(key_where, (count, STEPS), 0, 64) == 0
    depth_codes = jax.random.randint(key_depth, (count, STEPS), 768, 1025)
    kept_codes = jnp.where(lowered, depth_codes, 1024)
    codes = jnp.where(forgetful, plain_codes, kept_codes)
    return codes.reshape(-1).astype(jnp.int32)


def set_ends(values, rng, least, top_value):
    spot = [jax.random.randint(jax.random.fold_in(rng, axis), (), 0, length) for axis, length in enumerate(values.shape)]
    longest = values.shape.index(max(values.shape))
    beside = spot[:longest] + [(spot[longest] + 1) % values.shape[longest]] + spot[longest + 1:]
    return values.at[tuple(spot)].set(least).at[tuple(beside)].set(top_value)


def block_levels(key, extent, cuts, least, largest):
    level, own = 1.0, jax.random.fold_in(key, 6)
    for dim, shards_of in cuts:
        heights = jnp.exp(jax.random.uniform(jax.random.fold_in(own, dim), (shards_of,), jnp.float32, least / len(cuts), largest / len(cuts)))
        level = level * jnp.repeat(heights, extent[dim] // shards_of).reshape([-1 if axis == dim else 1 for axis in range(len(extent))])
    return level


def deal_out(stream_key, own, number, rows, count, top, most, skew):
    ranking = jax.random.permutation(stream_key, count)
    heavy_load, usual = portions_of(count, rows * top, most, skew, True), portions_of(count, rows * top, most, skew, False)
    places = jnp.arange(count)

    def named(lengths, turn):
        used = int((lengths > 0).sum())
        fixed = max(1, used // 4)
        passed = fixed + (places - fixed + turn * (used - fixed)) % max(1, count - fixed)
        return jnp.zeros((count,), jnp.int32).at[ranking[jnp.where(places < fixed, places, passed)]].set(jnp.asarray(lengths, jnp.int32))

    lengths = jnp.where(number % 4 == 0, named(heavy_load, number // 4), named(usual, number - number // 4 - 1))
    mixed = jax.random.permutation(jax.random.fold_in(own, 3), count)
    giver, receiver = mixed[0:count // 2 * 2:2], mixed[1:count // 2 * 2:2]
    room = jnp.minimum(lengths[giver] - 1, most - lengths[receiver]) // 2
    room = jnp.where((giver == ranking[0]) | (receiver == ranking[0]) | (lengths[receiver] == 0), 0, jnp.maximum(room, 0))
    passed = jax.random.randint(jax.random.fold_in(own, 4), (count // 2,), 0, 1 << 20) % (room + 1)
    lengths = lengths.at[giver].add(-passed).at[receiver].add(passed)
    items = jnp.searchsorted(jnp.cumsum(lengths), jnp.arange(rows * top), side="right").astype(jnp.int32)
    table = items.reshape(top, rows).T
    table = table[jax.random.permutation(jax.random.fold_in(own, 1), rows)]
    turn = jax.random.randint(jax.random.fold_in(own, 2), (rows, 1), 0, top)
    return jnp.take_along_axis(table, (jnp.arange(top)[None, :] + turn) % top, axis=1)


def portions_of(number_of, total, most, slope, full):
    loads = [(1 << 20) // math.isqrt(standing ** slope) + 1 for standing in range(1, number_of + 1)]
    largest = most if full else min(most, max(-(-total // number_of), total * loads[0] // sum(loads)))
    least = 1 if total - largest >= number_of - 1 else 0
    given, surplus = [largest] + [least] * (number_of - 1), total - largest - least * (number_of - 1)
    while surplus > 0:
        candidates = [i for i in range(1, number_of) if given[i] < largest] or [i for i in range(1, number_of) if given[i] < most]
        whole, remaining = sum([loads[i] for i in candidates]), surplus
        for i in candidates:
            addition = min(most - given[i], max(1, remaining * loads[i] // whole), surplus)
            given[i] = given[i] + addition
            surplus = surplus - addition
    return np.array(given)


def scatter_about(rng, extent, width, bound, shards=(), kind=jnp.bfloat16):
    values = jax.random.normal(rng, extent, jnp.float32) * width
    if len(shards) > 0:
        values = block_levels(rng, extent, shards, -0.22, 0.18) * values
    return jnp.clip(values, min=-bound, max=bound).astype(kind)


def setup_inputs(seed: int = 0) -> dict:
    key_list = jax.random.split(jax.random.key(seed), 12)
    tokens = scatter_about(key_list[0], (TOKENS, D), 1.0, 6.0, ((0, 64), (1, 2)))
    norm_gain = jnp.clip(1.0 + 0.15 * jax.random.normal(key_list[1], (D,), jnp.float32), 0.25, 1.75).astype(jnp.bfloat16)
    expert_ids_keys = jax.random.split(jax.random.fold_in(key_list[2], 1), TOKENS // TOK_GRP)
    expert_ids_turns = jax.random.permutation(jax.random.fold_in(key_list[2], 3), TOKENS // TOK_GRP)
    expert_ids = jax.vmap(lambda own, number: deal_out(jax.random.fold_in(key_list[2], 2), own, number, TOK_GRP, EXPERTS, TOP, CAP, 2))(expert_ids_keys, expert_ids_turns).reshape((TOKENS, TOP))
    gate_codes = set_ends(jax.random.randint(key_list[3], (TOKENS, TOP), 1, 256), jax.random.fold_in(key_list[3], 1), 1, 255).astype(jnp.int32)
    gate_weights = scatter_about(key_list[4], (EXPERTS, FF, D), D ** -0.5, 0.125, ((0, 4), (1, 32)))
    up_weights = scatter_about(key_list[5], (EXPERTS, FF, D), D ** -0.5, 0.125, ((0, 4), (1, 32)))
    down_weights = scatter_about(key_list[6], (EXPERTS, FF, D), FF ** -0.5, 0.0625, ((0, 4), (1, 32)))
    value_head = scatter_about(key_list[7], (D, NACT), D ** -0.5, 0.125)
    actions = set_ends(jax.random.randint(key_list[8], (TOKENS,), 0, NACT), jax.random.fold_in(key_list[8], 1), 0, NACT - 1).astype(jnp.int32)
    rewards = set_ends(jax.random.randint(key_list[9], (TOKENS,), -8, 9), jax.random.fold_in(key_list[9], 1), -8, 8).astype(jnp.int32)
    trace_codes = draw_trace_codes(jax.random.fold_in(key_list[11], 71), 0)
    return dict(tokens=tokens, norm_gain=norm_gain, expert_ids=expert_ids, gate_codes=gate_codes, gate_weights=gate_weights, up_weights=up_weights, down_weights=down_weights, value_head=value_head, actions=actions, rewards=rewards, trace_codes=trace_codes)


DISCOUNT = 0.99
EPSILON = 1e-05

def expert_rows(row_block, gate_matrix, lift_matrix, down_matrix):
    gate_value = lax.dot_general(row_block, gate_matrix, (((1,), (1,)), ((), ())), preferred_element_type=jnp.float32)
    lift_value = lax.dot_general(row_block, lift_matrix, (((1,), (1,)), ((), ())), preferred_element_type=jnp.float32)
    hidden = (jax.nn.silu(gate_value) * lift_value).astype(jnp.bfloat16)
    return jnp.dot(hidden, down_matrix, preferred_element_type=jnp.float32)

def retrace(action_values, actions, rewards, trace_codes):
    greedy = lax.optimization_barrier(jnp.max(action_values, axis=1))
    picked = (actions[:, None] == jnp.arange(action_values.shape[1], dtype=jnp.int32)[None, :]).astype(jnp.float32)
    taken = lax.optimization_barrier(jnp.sum(action_values * picked, axis=1))
    trace = trace_codes.astype(jnp.float32) / 1024.0
    reward = rewards.astype(jnp.float32) * 0.25
    greedy = greedy.reshape(-1, STEPS)
    taken = taken.reshape(-1, STEPS)
    trace = trace.reshape(-1, STEPS)
    reward = reward.reshape(-1, STEPS)
    padding = jnp.zeros_like(greedy[:, :1])
    greedy_next = jnp.concatenate([greedy[:, 1:], padding], axis=1)
    taken_next = jnp.concatenate([taken[:, 1:], padding], axis=1)
    trace_next = jnp.concatenate([trace[:, 1:], padding], axis=1)
    driver = reward + DISCOUNT * (greedy_next - trace_next * taken_next)
    log_sums = jnp.cumsum(jnp.log(DISCOUNT * trace), axis=1)
    spans = log_sums[:, None, :] - log_sums[:, :, None]
    upper_mask = jnp.arange(STEPS, dtype=jnp.int32)[None, :] >= jnp.arange(STEPS, dtype=jnp.int32)[:, None]
    weight = jnp.where(upper_mask[None, :, :], jnp.exp(jnp.minimum(spans, 0.0)), 0.0)
    target = jnp.einsum('nts,ns->nt', weight, driver, precision=lax.Precision.HIGHEST)
    return target.reshape(-1)

def reference(tokens, norm_gain, expert_ids, gate_codes, gate_weights, up_weights, down_weights, value_head, actions, rewards, trace_codes):
    widened = tokens.astype(jnp.float32)
    scaling = lax.rsqrt(lax.optimization_barrier(jnp.mean(widened * widened, axis=1, keepdims=True)) + EPSILON)
    normed = (widened * scaling * norm_gain.astype(jnp.float32)[None, :]).astype(jnp.bfloat16)
    codes = gate_codes.astype(jnp.float32)
    gate_share = codes / lax.optimization_barrier(jnp.sum(codes, axis=1, keepdims=True))
    row_limit = TOKENS // TOK_GRP * CAP

    def one_expert(running, inputs):
        expert_index, gate_matrix, lift_matrix, down_matrix = inputs
        matched = expert_ids == expert_index
        share = lax.optimization_barrier(jnp.sum(jnp.where(matched, gate_share, 0.0), axis=1))
        chosen = jnp.any(matched, axis=1)
        chosen_rows = jnp.nonzero(chosen, size=row_limit, fill_value=0)[0].astype(jnp.int32)
        amount = jnp.sum(chosen.astype(jnp.int32))
        in_range = (jnp.arange(row_limit, dtype=jnp.int32) < amount).astype(jnp.float32)
        output = expert_rows(normed[chosen_rows], gate_matrix, lift_matrix, down_matrix)
        running = running.at[chosen_rows].add(output * (share[chosen_rows] * in_range)[:, None])
        return (running, None)
    start_sum = jnp.zeros((TOKENS, D), jnp.float32)
    blended, _ = lax.scan(one_expert, start_sum, (jnp.arange(EXPERTS, dtype=jnp.int32), gate_weights, up_weights, down_weights))
    action_values = jnp.dot(blended, value_head.astype(jnp.float32), precision=lax.Precision.HIGHEST, preferred_element_type=jnp.float32)
    retrace_targets = retrace(action_values, actions, rewards, trace_codes)
    return (action_values, retrace_targets)
```

```python
import jax
import jax.numpy as jnp
from jax import lax
from jax.sharding import PartitionSpec as P

STEPS = 128
DISCOUNT = 0.99
EPSILON = 1e-05
HIGHEST = lax.Precision.HIGHEST


def retrace(action_values, actions, rewards, trace_codes):
    greedy = jnp.max(action_values, axis=1)
    picked = (
        actions[:, None] == jnp.arange(action_values.shape[1], dtype=jnp.int32)[None, :]
    ).astype(jnp.float32)
    taken = jnp.sum(action_values * picked, axis=1)
    trace = trace_codes.astype(jnp.float32) / 1024.0
    reward = rewards.astype(jnp.float32) * 0.25
    greedy = greedy.reshape(-1, STEPS)
    taken = taken.reshape(-1, STEPS)
    trace = trace.reshape(-1, STEPS)
    reward = reward.reshape(-1, STEPS)
    padding = jnp.zeros_like(greedy[:, :1])
    greedy_next = jnp.concatenate([greedy[:, 1:], padding], axis=1)
    taken_next = jnp.concatenate([taken[:, 1:], padding], axis=1)
    trace_next = jnp.concatenate([trace[:, 1:], padding], axis=1)
    driver = reward + DISCOUNT * (greedy_next - trace_next * taken_next)
    log_sums = jnp.cumsum(jnp.log(DISCOUNT * trace), axis=1)
    spans = log_sums[:, None, :] - log_sums[:, :, None]
    upper_mask = (
        jnp.arange(STEPS, dtype=jnp.int32)[None, :] >= jnp.arange(STEPS, dtype=jnp.int32)[:, None]
    )
    weight = jnp.where(upper_mask[None, :, :], jnp.exp(jnp.minimum(spans, 0.0)), 0.0)
    target = jnp.einsum("nts,ns->nt", weight, driver, precision=HIGHEST)
    return target.reshape(-1)


def rows_by(a, b):
    return lax.dot_general(a, b, (((1,), (1,)), ((), ())), preferred_element_type=jnp.float32)


def per_device(
    tokens,
    norm_gain,
    expert_ids,
    gate_codes,
    gate_weights,
    up_weights,
    down_weights,
    value_head,
    actions,
    rewards,
    trace_codes,
):
    dp, ex = lax.axis_size("dp"), lax.axis_size("expert")
    tp = lax.axis_size("tensor")
    rows, half = tokens.shape
    folded = jnp.dot(down_weights[0], value_head, preferred_element_type=jnp.float32)
    folded = folded.astype(jnp.bfloat16)
    wide = tokens.astype(jnp.float32)
    square = lax.psum(jnp.sum(wide * wide, axis=1, keepdims=True), "tensor") / (half * tp)
    gain = lax.dynamic_slice_in_dim(norm_gain, lax.axis_index("tensor") * half, half)
    normed = wide * lax.rsqrt(square + EPSILON) * gain.astype(jnp.float32)[None, :]
    normed = normed.astype(jnp.bfloat16)
    everyone = lax.all_gather(normed, ("dp", "expert", "tensor"), axis=0)
    everyone = everyone.reshape(dp * ex, tp, rows, half)
    left = everyone[:, 0].reshape(dp * ex * rows, half)
    right = everyone[:, 1].reshape(dp * ex * rows, half)
    gate_m, up_m = gate_weights[0], up_weights[0]
    gate = rows_by(left, gate_m[:, :half]) + rows_by(right, gate_m[:, half:])
    lift = rows_by(left, up_m[:, :half]) + rows_by(right, up_m[:, half:])
    hidden = (jax.nn.silu(gate) * lift).astype(jnp.bfloat16)
    value = jnp.dot(hidden, folded, preferred_element_type=jnp.float32)
    value = lax.psum_scatter(value, "dp", scatter_dimension=0, tiled=True)
    value = value.reshape(ex, rows, value.shape[1])
    value = lax.all_to_all(value, "expert", split_axis=0, concat_axis=0, tiled=True)
    codes = gate_codes.astype(jnp.float32)
    share = codes / jnp.sum(codes, axis=1, keepdims=True)
    named = expert_ids[None] == jnp.arange(ex, dtype=jnp.int32)[:, None, None]
    by_expert = jnp.sum(jnp.where(named, share[None], 0.0), axis=2)
    blended = jnp.sum(value * by_expert[:, :, None], axis=0)
    action_values = lax.psum(blended, "tensor")
    return action_values, retrace(action_values, actions, rewards, trace_codes)


def solution(mesh):
    group, weight = P(("dp", "expert"), None), P("expert", ("dp", "tensor"), None)
    line = P(("dp", "expert"))
    in_specs = (
        P(("dp", "expert"), "tensor"),
        P(),
        group,
        group,
        weight,
        weight,
        weight,
        P(),
        line,
        line,
        line,
    )
    return jax.shard_map(
        per_device, mesh=mesh, in_specs=in_specs, out_specs=(group, line), check_vma=False
    )
```

```python
import functools

import jax
import jax.numpy as jnp
from jax import lax
from jax.experimental import pallas as pl
from jax.experimental.pallas import tpu as pltpu
from jax.sharding import PartitionSpec as P

DISCOUNT = 0.99
EPSILON = 1e-05
MESH = pl.DeviceIdType.MESH
F32, BF16 = jnp.float32, jnp.bfloat16

OFFSET = (0, 3, 1, 2)
SEEN_AS = (0, 2, 1, 3)
ROW_A = 48
WEIGHT_ROWS = ((0, 32), (32, 64), (96, 64), (160, 64))


def rows_by(a, b):
    return lax.dot_general(a, b, (((1,), (1,)), ((), ())), preferred_element_type=F32)


def silu(v):
    return v / (1.0 + jnp.exp(-v))


def both(*key):
    return [(*key, 0), (*key, 1)]


def plan():
    first = [("w", 0)]
    first += [("r", 0, 1, 0, 0), ("r", 0, 2, 0, 1), ("r", 0, 0, 1, 0), ("r", 0, 0, 2, 1)]
    first += [("r", 0, 1, 0, 1), ("r", 0, 2, 0, 0), ("r", 0, 0, 1, 1), ("r", 0, 0, 2, 0)]
    first += [("r", 1, 0, 0, 0), ("r", 1, 0, 0, 1)]
    first += both("r", 0, 3, 0)
    first += [("r", 1, 1, 0, 0), ("r", 1, 2, 0, 1), ("r", 1, 1, 0, 1), ("r", 1, 2, 0, 0)]
    first += both("r", 0, 0, 3) + [("s", 0)]
    first += both("r", 1, 3, 0) + [("d",), ("p", 0)]

    def line(g, l):
        out = [("r", g, l, 1, 0), ("r", g, l, 2, 1), ("r", g, l, 1, 1), ("r", g, l, 2, 0)]
        return out + both("r", g, l, 3) + ([("s", l)] if g == 0 else [("b", l)])

    before_one = {0: first, 1: line(0, 1), 2: line(0, 2) + [("w", 1)], 3: line(0, 3)}
    before_one |= {4: line(1, 0), 5: line(1, 1) + [("w", 2)], 6: line(1, 2), 7: line(1, 3)}
    before_two = {0: [("p", 1)], 3: [("p", 2)], 8: [("w", 3), ("p", 3)]}
    return before_one, before_two


UNITS = ((0, 4), (1, 4), (2, 4), (0, 5), (1, 5), (2, 5), (3, 4), (3, 5), (0, 6), (1, 6), (2, 6), (3, 6))
UNITS_AFTER = {3: (0, 2), 5: (2, 5), 6: (5, 6), 7: (6, 12)}


def pick(index, values):
    out = values[-1]
    for i in range(len(values) - 2, -1, -1):
        out = jnp.where(index == i, values[i], out)
    return out


def kernel(
    tokens_ref,
    gain_ref,
    ids_ref,
    codes_ref,
    gate_ref,
    up_ref,
    down_ref,
    head_ref,
    actions_ref,
    rewards_ref,
    trace_ref,
    values_ref,
    targets_ref,
    tin,
    rin,
    tok,
    wb,
    down_v,
    head_v,
    folded,
    heads,
    acc,
    stage,
    parts,
    final,
    local_sem,
    raw_sem,
    tok_recv,
    tok_send,
    b_recv,
    b_send,
    w_recv,
    w_send,
    d_recv,
    d_send,
    rs_recv,
    rs_send,
    fin_sem,
):
    dp, z, c = lax.axis_index("dp"), lax.axis_index("expert"), lax.axis_index("tensor")
    x, y = dp % 4, dp // 4
    x_one = x + 1 - 2 * (x % 2)
    x_two = (x + 2 * (x % 2) + 3) % 4
    first, second = y * (1 - c) + z * c, z * (1 - c) + y * c

    def device(x_, f_, s_):
        y_, z_ = f_ * (1 - c) + s_ * c, s_ * (1 - c) + f_ * c
        return (y_ * 4 + x_, z_, c)

    partner = (dp, z, 1 - c)
    other = (y * 4 + x_one, z, c)
    twin = device(x_two, first, second)
    f_next = device(x, (first + 1) % 4, second)
    f_prev = device(x, (first + 3) % 4, second)
    s_next = device(x, first, (second + 1) % 4)
    s_prev = device(x, first, (second + 3) % 4)

    def remote(src, dst, send, recv, to):
        return pltpu.make_async_remote_copy(
            src_ref=src, dst_ref=dst, send_sem=send, recv_sem=recv, device_id=to, device_id_type=MESH
        )

    loads = [pltpu.make_async_copy(tokens_ref.at[pl.ds(i * 64, 64)], tin.at[i], local_sem.at[i]) for i in range(2)]
    w_loads = []
    for n, (at, size) in enumerate(WEIGHT_ROWS):
        chunk = n - 1 if n else 3
        for i, ref in enumerate((gate_ref, up_ref)):
            w_loads.append(
                pltpu.make_async_copy(
                    ref.at[0, pl.ds(at, size)], wb.at[chunk, pl.ds(i * 128, size)], local_sem.at[2 + 2 * n + i]
                )
            )
    d_loads = [
        pltpu.make_async_copy(down_ref.at[0], down_v, local_sem.at[10]),
        pltpu.make_async_copy(head_ref, head_v, local_sem.at[11]),
    ]
    for copy in loads + w_loads + d_loads:
        copy.start()

    barrier = pltpu.get_barrier_semaphore()
    count = 2
    for to in (partner, other):
        pl.semaphore_signal(barrier, inc=1, device_id=to, device_id_type=MESH)
    for g in range(2):
        for l in range(4):
            for s in range(4):
                if (g, l, s) == (0, 0, 0):
                    continue
                to = device(x_two if g else x, (first + OFFSET[l]) % 4, (second + OFFSET[s]) % 4)
                pl.semaphore_signal(barrier, inc=1, device_id=to, device_id_type=MESH)
                count += 1
    for copy in loads:
        copy.wait()
    pl.semaphore_wait(barrier, count)

    sends = []

    def start(make, *args):
        make(*args).start()
        sends.append((make, args))

    def raw_copy():
        return remote(tin.at[1 - c], rin, raw_sem.at[0], raw_sem.at[1], partner)

    start(raw_copy)
    for copy in w_loads:
        copy.wait()

    def weight_copy(n, i, role):
        size = WEIGHT_ROWS[n][1]
        mine, theirs = (n - 1, n + 3) if n else (3, 3)
        if role == 0:
            src, dst, at, to = mine, mine, (0, size), partner
        elif role == 1:
            src, dst, at, to = mine, theirs, (0, 0 if n else 2 * size), other
        else:
            src, dst, at, to = theirs, theirs, (0, size) if n else (2 * size, 3 * size), partner
        return remote(
            wb.at[src, pl.ds(i * 128 + at[0], size)],
            wb.at[dst, pl.ds(i * 128 + at[1], size)],
            w_send.at[role, n, i],
            w_recv.at[role, n, i],
            to,
        )

    for i in range(2):
        start(weight_copy, 0, i, 1)
    for n in range(4):
        for i in range(2):
            start(weight_copy, n, i, 0)

    raw_copy().wait_recv()
    mine = tin[c].astype(F32)
    theirs = rin[...].astype(F32)
    square = jnp.sum(mine * mine, axis=1, keepdims=True) + jnp.sum(theirs * theirs, axis=1, keepdims=True)
    scaling = lax.rsqrt(square / 2048.0 + EPSILON)
    for part, at in ((mine, c), (theirs, 1 - c)):
        lanes = pl.ds(pl.multiple_of(at * 1024, 1024), 1024)
        gain = gain_ref[:, lanes].astype(F32)
        tok[0, pl.ds(0, 64), lanes] = (part * scaling * gain).astype(BF16)

    def block(g, l, s, h):
        return tok.at[4 * g + l, pl.ds(64 * s, 64 if g == 0 else ROW_A), pl.ds(1024 * h, 1024)]

    def token_copy(g, src, dst, h, to):
        return remote(
            block(g, *src, h), block(g, *dst, h), tok_send.at[g, *dst, h], tok_recv.at[g, *dst, h], to
        )

    def along_second(g, l, h):
        start(token_copy, g, (l, 0), (l, 1), h, s_next)
        start(token_copy, g, (l, 0), (l, 2), h, s_prev)

    def along_first(g, h, up):
        if up:
            start(token_copy, g, (0, 0), (1, 0), h, f_next)
        else:
            start(token_copy, g, (0, 0), (2, 0), h, f_prev)

    def edge(ref, l, s):
        return ref.at[l, pl.ds(64 * s + ROW_A, 64 - ROW_A)]

    def edge_copy(l, s):
        return remote(edge(tok, l, s), edge(tok, 4 + l, s), b_send.at[l, s], b_recv.at[l, s], twin)

    def twin_copy(h):
        src = tok.at[0, pl.ds(0, ROW_A), pl.ds(1024 * h, 1024)]
        return remote(src, block(1, 0, 0, h), tok_send.at[1, 0, 0, h], tok_recv.at[1, 0, 0, h], twin)

    for h in range(2):
        along_first(0, h, True)
        along_first(0, 1 - h, False)
        start(twin_copy, h)
        start(token_copy, 0, (0, 0), (0, 1), h, s_next)
        start(token_copy, 0, (0, 0), (0, 2), 1 - h, s_prev)
    start(edge_copy, 0, 0)

    for copy in d_loads:
        copy.wait()
    folded[0] = jnp.dot(down_v[...], head_v[...], preferred_element_type=F32).astype(BF16)

    def head_copy(role):
        src, dst, to = ((0, 1, partner), (0, 2, other), (2, 3, partner))[role]
        return remote(folded.at[src], folded.at[dst], d_send.at[role], d_recv.at[role], to)

    start(head_copy, 1)
    start(head_copy, 0)
    for n in range(1, 4):
        for i in range(2):
            start(weight_copy, n, i, 1)

    def happen(event):
        kind = event[0]
        if kind == "r":
            _, g, l, s, h = event
            copy = token_copy(g, (l, s), (l, s), h, partner)
            copy.wait_recv()
            if s == 0:
                if l == 0:
                    along_first(g, h, True)
                    along_first(g, h, False)
                if (l, h) == (1, 0):
                    start(token_copy, g, (1, 0), (3, 0), 0, f_next)
                if (l, h) == (2, 1):
                    start(token_copy, g, (2, 0), (3, 0), 1, f_prev)
                along_second(g, l, h)
            if (s, h) == (1, 0):
                start(token_copy, g, (l, 1), (l, 3), 0, s_next)
            if (s, h) == (2, 1):
                start(token_copy, g, (l, 2), (l, 3), 1, s_prev)
        elif kind == "s":
            for s in range(4):
                if (event[1], s) != (0, 0):
                    start(edge_copy, event[1], s)
        elif kind == "b":
            for s in range(4):
                edge_copy(event[1], s).wait_recv()
        elif kind == "w":
            for i in range(2):
                weight_copy(event[1], i, 1).wait_recv()
                start(weight_copy, event[1], i, 2)
        elif kind == "p":
            for i in range(2):
                weight_copy(event[1], i, 2).wait_recv()
        else:
            head_copy(1).wait_recv()
            start(head_copy, 2)
            head_copy(0).wait_recv()
            head_copy(2).wait_recv()
            for n in range(4):
                at, size = WEIGHT_ROWS[n]
                if n == 0:
                    for j in range(4):
                        heads[3, pl.ds(32 * j, 32)] = folded[j, pl.ds(at, size)]
                else:
                    for j in range(4):
                        heads[n - 1 + 4 * (j // 2), pl.ds(64 * (j % 2), 64)] = folded[j, pl.ds(at, size)]

    before_one, before_two = plan()
    for n in range(4):
        for i in range(2):
            weight_copy(n, i, 0).wait_recv()
    for event in before_one[0]:
        happen(event)

    def unit_one(b):
        product = rows_by(tok[b], wb[0:4].reshape(1024, 2048))
        hidden = [
            (silu(product[:, 256 * k : 256 * k + 128]) * product[:, 256 * k + 128 : 256 * k + 256]).astype(BF16)
            for k in range(4)
        ]
        acc[pl.ds(pl.multiple_of(256 * b, 256), 256)] = jnp.dot(
            jnp.concatenate(hidden, axis=1), heads[0:4].reshape(512, 128), preferred_element_type=F32
        )

    def unit_two(p, k):
        product = rows_by(tok[pl.ds(2 * p, 2)].reshape(512, 2048), wb[k])
        hidden = (silu(product[:, :128]) * product[:, 128:]).astype(BF16)
        rows = pl.ds(pl.multiple_of(512 * p, 512), 512)
        total = acc[rows] + jnp.dot(hidden, heads[k], preferred_element_type=F32)
        acc[rows] = total
        return total

    def part_copy(p, r, s):
        g, q = p // 2, p % 2
        to = device(
            x + g * (x_two - x), (first + q + r * (3 - 2 * q)) % 4, (second + OFFSET[s]) % 4
        )
        src = stage.at[2 * p + r, pl.ds(64 * s, 64)]
        slot = g * 16 + (q + 2 * r) * 4 + SEEN_AS[s]
        return remote(src, parts.at[slot], rs_send.at[slot], rs_recv.at[slot], to)

    def step(j, _):
        for i in range(1, 8):

            @pl.when(j == i)
            def _():
                for event in before_one[i]:
                    happen(event)

        unit_one(j)

        def inner(u, _):
            for i, events in before_two.items():

                @pl.when(u == i)
                def _():
                    for event in events:
                        happen(event)

            p, k = pick(u, [v[0] for v in UNITS]), pick(u, [v[1] for v in UNITS])
            total = unit_two(p, k)

            @pl.when(u >= 8)
            def _():
                stage[pl.ds(2 * p, 2)] = total.astype(BF16).reshape(2, 256, 128)
                for r in range(2):
                    for s in range(4):
                        if (r, s) == (0, 0):

                            @pl.when(p > 0)
                            def _():
                                part_copy(p, 0, 0).start()

                        else:
                            part_copy(p, r, s).start()

            return 0

        low = pick(j, [UNITS_AFTER.get(i, (0, 0))[0] for i in range(8)])
        high = pick(j, [UNITS_AFTER.get(i, (0, 0))[1] for i in range(8)])
        lax.fori_loop(low, high, inner, 0)
        return 0

    lax.fori_loop(0, 8, step, 0)

    codes = codes_ref[pl.ds(pl.multiple_of(64 * c, 64), 64), :].astype(F32)
    ids = ids_ref[pl.ds(pl.multiple_of(64 * c, 64), 64), :]
    share = codes / (codes[:, 0:1] + codes[:, 1:2])
    shares = []
    for j in range(4):
        named = ids == (z + OFFSET[j]) % 4
        picked = jnp.where(named, share, 0.0)
        shares.append(picked[:, 0:1] + picked[:, 1:2])
    c_wide = c.astype(F32)

    for slot in range(1, 32):
        remote(parts.at[slot], parts.at[slot], rs_send.at[slot], rs_recv.at[slot], partner).wait_recv()
    blended = jnp.zeros((64, 128), F32)
    for l in range(4):
        for s in range(4):
            slot = 4 * l + s
            near = parts[slot].astype(F32) if slot else acc[0:64]
            weight = shares[s] * (1.0 - c_wide) + shares[l] * c_wide
            blended += (near + parts[16 + slot].astype(F32)) * weight
    final[c] = blended

    def final_copy():
        return remote(final.at[c], final.at[c], fin_sem.at[0], fin_sem.at[1], partner)

    start(final_copy)
    final_copy().wait_recv()
    values = final[...].reshape(128, 128)
    values_ref[...] = values

    lane = lax.broadcasted_iota(jnp.int32, (128, 128), 1)
    row = lax.broadcasted_iota(jnp.int32, (128, 128), 0)

    def column(v):
        return jnp.sum(jnp.where(lane == row, v, 0.0), axis=1, keepdims=True)

    trace = trace_ref[...].astype(F32) / 1024.0
    reward = rewards_ref[...].astype(F32) * 0.25
    action_column = jnp.sum(jnp.where(lane == row, actions_ref[...], 0), axis=1, keepdims=True)
    greedy = jnp.max(values, axis=1, keepdims=True)
    taken = jnp.sum(jnp.where(lane == action_column, values, 0.0), axis=1, keepdims=True)
    ahead = greedy - column(trace) * taken
    driver = reward + DISCOUNT * jnp.sum(jnp.where(row == lane + 1, ahead, 0.0), axis=0, keepdims=True)
    logs = jnp.log(DISCOUNT * trace)
    sums_column = jnp.sum(jnp.where(lane <= row, logs, 0.0), axis=1, keepdims=True)
    sums_row = jnp.sum(jnp.where(lane == row, sums_column, 0.0), axis=0, keepdims=True)
    weight = jnp.where(lane >= row, jnp.exp(jnp.minimum(sums_row - sums_column, 0.0)), 0.0)
    target = jnp.sum(weight * driver, axis=1, keepdims=True)
    targets_ref[...] = jnp.sum(jnp.where(lane == row, target, 0.0), axis=0, keepdims=True)

    for make, args in sends:
        make(*args).wait_send()
    for slot in range(1, 32):
        remote(parts.at[slot], parts.at[slot], rs_send.at[slot], rs_recv.at[slot], partner).wait_send()


def per_device(
    tokens,
    norm_gain,
    expert_ids,
    gate_codes,
    gate_weights,
    up_weights,
    down_weights,
    value_head,
    actions,
    rewards,
    trace_codes,
):
    dma = pltpu.SemaphoreType.DMA
    vmem, hbm = pl.BlockSpec(memory_space=pltpu.VMEM), pl.BlockSpec(memory_space=pl.ANY)
    values, targets = pl.pallas_call(
        kernel,
        out_shape=(jax.ShapeDtypeStruct((128, 128), F32), jax.ShapeDtypeStruct((1, 128), F32)),
        in_specs=[hbm, vmem, vmem, vmem, hbm, hbm, hbm, hbm, vmem, vmem, vmem],
        out_specs=(vmem, vmem),
        scratch_shapes=[
            pltpu.VMEM((2, 64, 1024), BF16),
            pltpu.VMEM((64, 1024), BF16),
            pltpu.VMEM((8, 256, 2048), BF16),
            pltpu.VMEM((7, 256, 2048), BF16),
            pltpu.VMEM((224, 2048), BF16),
            pltpu.VMEM((2048, 128), BF16),
            pltpu.VMEM((4, 224, 128), BF16),
            pltpu.VMEM((7, 128, 128), BF16),
            pltpu.VMEM((2048, 128), F32),
            pltpu.VMEM((8, 256, 128), BF16),
            pltpu.VMEM((32, 64, 128), BF16),
            pltpu.VMEM((2, 64, 128), F32),
            dma((12,)),
            dma((2,)),
            dma((2, 4, 4, 2)),
            dma((2, 4, 4, 2)),
            dma((4, 4)),
            dma((4, 4)),
            dma((3, 4, 2)),
            dma((3, 4, 2)),
            dma((3,)),
            dma((3,)),
            dma((32,)),
            dma((32,)),
            dma((2,)),
        ],
        compiler_params=pltpu.CompilerParams(
            collective_id=0, has_side_effects=True, vmem_limit_bytes=56 * 1024 * 1024
        ),
        name="critic",
    )(
        tokens,
        norm_gain.reshape(1, -1),
        expert_ids,
        gate_codes,
        gate_weights,
        up_weights,
        down_weights,
        value_head,
        actions.reshape(1, -1),
        rewards.reshape(1, -1),
        trace_codes.reshape(1, -1),
    )
    return values, targets.reshape(-1)


def solution(mesh):
    group, weight = P(("dp", "expert"), None), P("expert", ("dp", "tensor"), None)
    line = P(("dp", "expert"))
    in_specs = (
        P(("dp", "expert"), "tensor"),
        P(),
        group,
        group,
        weight,
        weight,
        weight,
        P(),
        line,
        line,
        line,
    )
    return jax.shard_map(
        per_device, mesh=mesh, in_specs=in_specs, out_specs=(group, line), check_vma=False
    )
```

```python
import functools

import jax
import jax.numpy as jnp
from jax import lax
from jax.experimental import pallas as pl
from jax.experimental.pallas import tpu as pltpu
from jax.sharding import PartitionSpec as P

DISCOUNT = 0.99
EPSILON = 1e-05
MESH = pl.DeviceIdType.MESH
F32, BF16 = jnp.float32, jnp.bfloat16

OFFSET = (0, 3, 1, 2)
SEEN_AS = (0, 2, 1, 3)
ROW_A = 48
WEIGHT_ROWS = ((0, 32), (32, 64), (96, 64), (160, 64))


def rows_by(a, b):
    return lax.dot_general(a, b, (((1,), (1,)), ((), ())), preferred_element_type=F32)


def silu(v):
    return v / (1.0 + jnp.exp(-v))


ORDER = (
    (
        (
            ("r", 1, 0, 0, 0), ("q", 1, 0, 0), ("r", 0, 1, 0, 0), ("q", 0, 1, 0), ("r", 0, 2, 0, 1),
            ("r", 0, 0, 1, 0), ("r", 0, 0, 2, 1), ("r", 1, 0, 0, 1), ("f", 0, 0, 0), ("f", 0, 0, 1),
            ("r", 0, 1, 0, 1), ("e", 1, 0), ("r", 0, 2, 0, 0), ("e", 2, 0), ("r", 0, 0, 1, 1), ("e", 0, 1),
            ("r", 0, 0, 2, 0), ("e", 0, 2), ("w", 0), ("B", 0, 0), ("w", "d"), ("q", 0, 1, 1), ("p", 0),
            ("r", 1, 1, 0, 0), ("r", 1, 2, 0, 0), ("r", 1, 0, 1, 0), ("r", 1, 0, 2, 0), ("p", "d"),
            ("B", 1, 0), ("q", 0, 2, 1), ("B", 2, 0), ("r", 0, 3, 0, 0), ("r", 0, 3, 0, 1), ("e", 3, 0),
            ("r", 0, 1, 1, 0), ("r", 0, 1, 2, 0), ("B", 0, 1), ("r", 1, 1, 0, 1), ("r", 1, 2, 0, 1),
            ("q", 0, 2, 0), ("r", 0, 0, 3, 1), ("B", 0, 2), ("r", 0, 0, 3, 0), ("e", 0, 3),
        ),
        (0,),
    ),
    (
        (
            ("f", 0, 1, 0), ("r", 0, 1, 2, 1), ("e", 1, 2), ("f", 0, 1, 1), ("B", 3, 0), ("r", 1, 3, 0, 0),
            ("r", 0, 1, 1, 1), ("e", 1, 1), ("q", 0, 3, 0), ("B", 0, 3), ("r", 1, 3, 0, 1), ("r", 0, 2, 1, 1),
            ("r", 0, 2, 2, 1), ("q", 0, 3, 1), ("w", 1), ("B", 1, 2), ("r", 0, 2, 1, 0), ("e", 2, 1),
            ("r", 0, 2, 2, 0), ("e", 2, 2), ("f", 0, 2, 1), ("f", 0, 2, 0), ("B", 1, 1), ("r", 0, 1, 3, 0),
            ("r", 0, 1, 3, 1), ("e", 1, 3),
        ),
        (1,),
    ),
    (
        (
            ("q", 1, 0, 1), ("q", 1, 1, 0), ("p", 1), ("r", 0, 3, 1, 0), ("r", 0, 3, 2, 0),
        ),
        (0, 4),
    ),
    (
        (
            ("f", 0, 3, 0), ("B", 2, 1), ("r", 0, 3, 1, 1), ("e", 3, 1), ("r", 0, 3, 2, 1), ("e", 3, 2),
            ("f", 0, 3, 1), ("B", 2, 2), ("q", 1, 1, 1), ("r", 0, 2, 3, 0), ("r", 0, 2, 3, 1), ("e", 2, 3),
        ),
        (2,),
    ),
    (
        (
            ("f", 1, 0, 0), ("q", 1, 2, 0), ("B", 1, 3), ("r", 1, 0, 1, 1), ("r", 1, 0, 2, 1), ("f", 1, 0, 1),
            ("B", 3, 1), ("r", 1, 1, 1, 0), ("r", 1, 1, 2, 0), ("q", 1, 2, 1), ("B", 3, 2), ("r", 0, 3, 3, 0),
            ("r", 0, 3, 3, 1), ("e", 3, 3),
        ),
        (3,),
    ),
    (
        (
            ("f", 1, 1, 0), ("q", 1, 3, 0), ("r", 1, 1, 1, 1), ("r", 1, 1, 2, 1), ("f", 1, 1, 1), ("B", 2, 3),
        ),
        (1, 4),
    ),
    (
        (
            ("q", 1, 3, 1), ("w", 2), ("r", 1, 0, 3, 0), ("r", 1, 2, 2, 0), ("r", 1, 2, 1, 0),
            ("r", 1, 0, 3, 1),
        ),
        (4,),
    ),
    (
        (
            ("f", 1, 2, 0), ("B", 3, 3), ("r", 1, 2, 1, 1), ("r", 1, 2, 2, 1), ("f", 1, 2, 1), ("p", 2),
        ),
        (0, 5),
    ),
    (
        (
            ("r", 1, 1, 3, 0), ("r", 1, 3, 2, 0),
        ),
        (1, 5),
    ),
    (
        (
            ("r", 1, 3, 1, 0), ("f", 1, 3, 0), ("r", 1, 1, 3, 1),
        ),
        (5,),
    ),
    (
        (
            ("r", 1, 3, 1, 1), ("r", 1, 3, 2, 1), ("f", 1, 3, 1), ("r", 1, 2, 3, 0), ("r", 1, 2, 3, 1),
        ),
        (6,),
    ),
    (
        (
            ("r", 1, 3, 3, 0),
        ),
        (2, 4),
    ),
    (
        (
        ),
        (2, 5),
    ),
    (
        (
            ("r", 1, 3, 3, 1),
        ),
        (7,),
    ),
    (
        (
            ("w", 3),
        ),
        (3, 4),
    ),
    (
        (
        ),
        (3, 5),
    ),
    (
        (
            ("p", 3),
        ),
        (0, 6),
    ),
    (
        (
        ),
        (1, 6),
    ),
    (
        (
        ),
        (2, 6),
    ),
    (
        (
        ),
        (3, 6),
    ),
)


def pick(index, values):
    out = values[-1]
    for i in range(len(values) - 2, -1, -1):
        out = jnp.where(index == i, values[i], out)
    return out


def kernel(
    tokens_ref,
    gain_ref,
    ids_ref,
    codes_ref,
    gate_ref,
    up_ref,
    down_ref,
    head_ref,
    final_ref,
    tin,
    rin,
    tok,
    wb,
    down_v,
    head_v,
    folded,
    heads,
    acc,
    stage,
    parts,
    gain_v,
    local_sem,
    raw_sem,
    tok_recv,
    tok_send,
    b_recv,
    b_send,
    w_recv,
    w_send,
    d_recv,
    d_send,
    rs_recv,
    rs_send,
    fin_sem,
):
    dp, z, c = lax.axis_index("dp"), lax.axis_index("expert"), lax.axis_index("tensor")
    x, y = dp % 4, dp // 4
    x_one = x + 1 - 2 * (x % 2)
    x_two = (x + 2 * (x % 2) + 3) % 4
    first, second = y * (1 - c) + z * c, z * (1 - c) + y * c

    def device(x_, f_, s_):
        y_, z_ = f_ * (1 - c) + s_ * c, s_ * (1 - c) + f_ * c
        return (y_ * 4 + x_, z_, c)

    partner = (dp, z, 1 - c)
    other = (y * 4 + x_one, z, c)
    twin = device(x_two, first, second)
    f_next = device(x, (first + 1) % 4, second)
    f_prev = device(x, (first + 3) % 4, second)
    s_next = device(x, first, (second + 1) % 4)
    s_prev = device(x, first, (second + 3) % 4)

    def remote(src, dst, send, recv, to):
        return pltpu.make_async_remote_copy(
            src_ref=src, dst_ref=dst, send_sem=send, recv_sem=recv, device_id=to, device_id_type=MESH
        )

    loads = [pltpu.make_async_copy(tokens_ref.at[pl.ds(i * 64, 64)], tin.at[i], local_sem.at[i]) for i in range(2)]
    w_loads = []
    for n, (at, size) in enumerate(WEIGHT_ROWS):
        chunk = n - 1 if n else 3
        for i, ref in enumerate((gate_ref, up_ref)):
            w_loads.append(
                pltpu.make_async_copy(
                    ref.at[0, pl.ds(at, size)], wb.at[chunk, pl.ds(i * 128, size)], local_sem.at[2 + 2 * n + i]
                )
            )
    d_loads = [
        pltpu.make_async_copy(down_ref.at[0], down_v, local_sem.at[10]),
        pltpu.make_async_copy(head_ref, head_v, local_sem.at[11]),
    ]
    for copy in loads + w_loads + d_loads:
        copy.start()

    barrier = pltpu.get_barrier_semaphore()
    for to in (partner, other, twin, f_next, f_prev, s_next, s_prev):
        pl.semaphore_signal(barrier, inc=1, device_id=to, device_id_type=MESH)
    for copy in loads:
        copy.wait()
    pl.semaphore_wait(barrier, 7)

    sends = []

    def start(make, *args):
        make(*args).start()
        sends.append((make, args))

    def raw_copy():
        return remote(tin.at[1 - c], rin, raw_sem.at[0], raw_sem.at[1], partner)

    start(raw_copy)
    for copy in w_loads:
        copy.wait()

    def weight_copy(n, i, role):
        size = WEIGHT_ROWS[n][1]
        mine, theirs = (n - 1, n + 3) if n else (3, 3)
        if role == 0:
            src, dst, at, to = mine, mine, (0, size), partner
        elif role == 1:
            src, dst, at, to = mine, theirs, (0, 0 if n else 2 * size), other
        else:
            src, dst, at, to = theirs, theirs, (0, size) if n else (2 * size, 3 * size), partner
        return remote(
            wb.at[src, pl.ds(i * 128 + at[0], size)],
            wb.at[dst, pl.ds(i * 128 + at[1], size)],
            w_send.at[role, n, i],
            w_recv.at[role, n, i],
            to,
        )

    for i in range(2):
        start(weight_copy, 0, i, 1)
    for n in range(4):
        for i in range(2):
            start(weight_copy, n, i, 0)

    raw_copy().wait_recv()
    mine = tin[c].astype(F32)
    theirs = rin[...].astype(F32)
    square = jnp.sum(mine * mine, axis=1, keepdims=True) + jnp.sum(theirs * theirs, axis=1, keepdims=True)
    scaling = lax.rsqrt(square / 2048.0 + EPSILON)
    gain_v[...] = gain_ref[...].astype(F32)
    for part, at in ((mine, c), (theirs, 1 - c)):
        for i in range(8):
            lanes = pl.ds(pl.multiple_of(at * 1024 + 128 * i, 128), 128)
            gain = gain_v[pl.ds(8 * at + i, 1), :]
            tok[0, pl.ds(0, 64), lanes] = (part[:, 128 * i : 128 * i + 128] * scaling * gain).astype(BF16)

    def block(g, l, s, h):
        return tok.at[4 * g + l, pl.ds(64 * s, 64 if g == 0 else ROW_A), pl.ds(1024 * h, 1024)]

    def token_copy(g, src, dst, h, to):
        return remote(
            block(g, *src, h), block(g, *dst, h), tok_send.at[g, *dst, h], tok_recv.at[g, *dst, h], to
        )

    def along_second(g, l, h):
        start(token_copy, g, (l, 0), (l, 1), h, s_next)
        start(token_copy, g, (l, 0), (l, 2), h, s_prev)

    def along_first(g, h, up):
        if up:
            start(token_copy, g, (0, 0), (1, 0), h, f_next)
        else:
            start(token_copy, g, (0, 0), (2, 0), h, f_prev)

    def edge(ref, l, s):
        return ref.at[l, pl.ds(64 * s + ROW_A, 64 - ROW_A)]

    def edge_copy(l, s):
        return remote(edge(tok, l, s), edge(tok, 4 + l, s), b_send.at[l, s], b_recv.at[l, s], twin)

    def twin_copy(h):
        src = tok.at[0, pl.ds(0, ROW_A), pl.ds(1024 * h, 1024)]
        return remote(src, block(1, 0, 0, h), tok_send.at[1, 0, 0, h], tok_recv.at[1, 0, 0, h], twin)

    for h in range(2):
        along_first(0, h, True)
        along_first(0, 1 - h, False)
        start(twin_copy, h)
        start(token_copy, 0, (0, 0), (0, 1), h, s_next)
        start(token_copy, 0, (0, 0), (0, 2), 1 - h, s_prev)
    start(edge_copy, 0, 0)

    for copy in d_loads:
        copy.wait()
    folded[0] = jnp.dot(down_v[...], head_v[...], preferred_element_type=F32).astype(BF16)

    def head_copy(role):
        src, dst, to = ((0, 1, partner), (0, 2, other), (2, 3, partner))[role]
        return remote(folded.at[src], folded.at[dst], d_send.at[role], d_recv.at[role], to)

    start(head_copy, 1)
    start(head_copy, 0)
    for n in range(1, 4):
        for i in range(2):
            start(weight_copy, n, i, 1)

    def happen(event):
        kind = event[0]
        if kind == "r":
            _, g, l, s, h = event
            token_copy(g, (l, s), (l, s), h, partner).wait_recv()
            if s == 0:
                if l == 0:
                    along_first(g, h, True)
                    along_first(g, h, False)
                if (l, h) == (1, 0):
                    start(token_copy, g, (1, 0), (3, 0), 0, f_next)
                if (l, h) == (2, 1):
                    start(token_copy, g, (2, 0), (3, 0), 1, f_prev)
        elif kind == "q":
            along_second(*event[1:])
        elif kind == "f":
            _, g, l, h = event
            start(token_copy, g, (l, 1 + h), (l, 3), h, s_prev if h else s_next)
        elif kind == "e":
            start(edge_copy, event[1], event[2])
        elif kind == "B":
            edge_copy(event[1], event[2]).wait_recv()
        elif kind == "w":
            if event[1] == "d":
                head_copy(1).wait_recv()
                start(head_copy, 2)
            else:
                for i in range(2):
                    weight_copy(event[1], i, 1).wait_recv()
                    start(weight_copy, event[1], i, 2)
        elif event[1] != "d":
            for i in range(2):
                weight_copy(event[1], i, 2).wait_recv()
        else:
            head_copy(0).wait_recv()
            head_copy(2).wait_recv()
            for n in range(4):
                at, size = WEIGHT_ROWS[n]
                for j in range(4):
                    if n == 0:
                        heads[3, pl.ds(32 * j, 32)] = folded[j, pl.ds(at, size)]
                    else:
                        heads[n - 1 + 4 * (j // 2), pl.ds(64 * (j % 2), 64)] = folded[j, pl.ds(at, size)]

    for n in range(4):
        for i in range(2):
            weight_copy(n, i, 0).wait_recv()

    def unit_one(b):
        product = rows_by(tok[b], wb[0:4].reshape(1024, 2048))
        hidden = [
            (silu(product[:, 256 * k : 256 * k + 128]) * product[:, 256 * k + 128 : 256 * k + 256]).astype(BF16)
            for k in range(4)
        ]
        acc[pl.ds(pl.multiple_of(256 * b, 256), 256)] = jnp.dot(
            jnp.concatenate(hidden, axis=1), heads[0:4].reshape(512, 128), preferred_element_type=F32
        )

    def unit_two(p, k):
        product = rows_by(tok[pl.ds(2 * p, 2)].reshape(512, 2048), wb[k])
        hidden = (silu(product[:, :128]) * product[:, 128:]).astype(BF16)
        rows = pl.ds(pl.multiple_of(512 * p, 512), 512)
        total = acc[rows] + jnp.dot(hidden, heads[k], preferred_element_type=F32)
        acc[rows] = total
        return total

    def part_copy(p, r, s):
        g, q = p // 2, p % 2
        to = device(
            x + g * (x_two - x), (first + q + r * (3 - 2 * q)) % 4, (second + OFFSET[s]) % 4
        )
        src = stage.at[2 * p + r, pl.ds(64 * s, 64)]
        slot = g * 16 + (q + 2 * r) * 4 + SEEN_AS[s]
        return remote(src, parts.at[slot], rs_send.at[slot], rs_recv.at[slot], to)

    def step(u, _):
        for i, (events, _) in enumerate(ORDER):
            if events:

                @pl.when(u == i)
                def _():
                    for event in events:
                        happen(event)

        wide = pick(u, [int(len(unit) == 1) for _, unit in ORDER])
        p = pick(u, [unit[0] for _, unit in ORDER])
        k = pick(u, [unit[-1] for _, unit in ORDER])

        @pl.when(wide == 1)
        def _():
            unit_one(p)

        @pl.when(wide == 0)
        def _():
            total = unit_two(p, k)

            @pl.when(k == 6)
            def _():
                stage[pl.ds(2 * p, 2)] = total.astype(BF16).reshape(2, 256, 128)
                for r in range(2):
                    for s in range(4):
                        if (r, s) == (0, 0):

                            @pl.when(p > 0)
                            def _():
                                part_copy(p, 0, 0).start()

                        else:
                            part_copy(p, r, s).start()

        return 0

    lax.fori_loop(0, len(ORDER), step, 0)

    spot = lax.broadcasted_iota(jnp.int32, (64, 128), 1) == lax.broadcasted_iota(jnp.int32, (64, 128), 0) + 64 * c

    def upright(ref, i):
        return jnp.sum(jnp.where(spot, ref[i : i + 1, :], 0), axis=1, keepdims=True)

    ids = [upright(ids_ref, i) for i in range(2)]
    codes = [upright(codes_ref, i).astype(F32) for i in range(2)]
    share = [code / (codes[0] + codes[1]) for code in codes]
    shares = []
    for j in range(4):
        e = (z + OFFSET[j]) % 4
        shares.append(jnp.where(ids[0] == e, share[0], 0.0) + jnp.where(ids[1] == e, share[1], 0.0))
    c_wide = c.astype(F32)

    for slot in range(1, 32):
        remote(parts.at[slot], parts.at[slot], rs_send.at[slot], rs_recv.at[slot], partner).wait_recv()
    blended = jnp.zeros((64, 128), F32)
    for l in range(4):
        for s in range(4):
            slot = 4 * l + s
            near = parts[slot].astype(F32) if slot else acc[0:64]
            weight = shares[s] * (1.0 - c_wide) + shares[l] * c_wide
            blended += (near + parts[16 + slot].astype(F32)) * weight
    rows = pl.ds(pl.multiple_of(64 * c, 64), 64)
    final_ref[rows] = blended

    def final_copy():
        return remote(final_ref.at[rows], final_ref.at[rows], fin_sem.at[0], fin_sem.at[1], partner)

    start(final_copy)
    final_copy().wait_recv()

    for make, args in sends:
        make(*args).wait_send()
    for slot in range(1, 32):
        remote(parts.at[slot], parts.at[slot], rs_send.at[slot], rs_recv.at[slot], partner).wait_send()


def last_kernel(final_ref, actions_ref, rewards_ref, trace_ref, values_ref, targets_ref):
    values = final_ref[...]
    values_ref[...] = values
    lane = lax.broadcasted_iota(jnp.int32, (128, 128), 1)
    row = lax.broadcasted_iota(jnp.int32, (128, 128), 0)

    def column(v):
        return jnp.sum(jnp.where(lane == row, v, 0.0), axis=1, keepdims=True)

    trace = trace_ref[...].astype(F32) / 1024.0
    reward = rewards_ref[...].astype(F32) * 0.25
    action_column = jnp.sum(jnp.where(lane == row, actions_ref[...], 0), axis=1, keepdims=True)
    greedy = jnp.max(values, axis=1, keepdims=True)
    taken = jnp.sum(jnp.where(lane == action_column, values, 0.0), axis=1, keepdims=True)
    ahead = greedy - column(trace) * taken
    driver = reward + DISCOUNT * jnp.sum(jnp.where(row == lane + 1, ahead, 0.0), axis=0, keepdims=True)
    logs = jnp.log(DISCOUNT * trace)
    sums_column = jnp.sum(jnp.where(lane <= row, logs, 0.0), axis=1, keepdims=True)
    sums_row = jnp.sum(jnp.where(lane == row, sums_column, 0.0), axis=0, keepdims=True)
    weight = jnp.where(lane >= row, jnp.exp(jnp.minimum(sums_row - sums_column, 0.0)), 0.0)
    target = jnp.sum(weight * driver, axis=1, keepdims=True)
    targets_ref[...] = jnp.sum(jnp.where(lane == row, target, 0.0), axis=0, keepdims=True)


def per_device(
    tokens,
    norm_gain,
    expert_ids,
    gate_codes,
    gate_weights,
    up_weights,
    down_weights,
    value_head,
    actions,
    rewards,
    trace_codes,
):
    dma = pltpu.SemaphoreType.DMA
    vmem, hbm = pl.BlockSpec(memory_space=pltpu.VMEM), pl.BlockSpec(memory_space=pl.ANY)
    final = pl.pallas_call(
        kernel,
        out_shape=jax.ShapeDtypeStruct((128, 128), F32),
        in_specs=[hbm, vmem, vmem, vmem, hbm, hbm, hbm, hbm],
        out_specs=vmem,
        scratch_shapes=[
            pltpu.VMEM((2, 64, 1024), BF16),
            pltpu.VMEM((64, 1024), BF16),
            pltpu.VMEM((8, 256, 2048), BF16),
            pltpu.VMEM((7, 256, 2048), BF16),
            pltpu.VMEM((224, 2048), BF16),
            pltpu.VMEM((2048, 128), BF16),
            pltpu.VMEM((4, 224, 128), BF16),
            pltpu.VMEM((7, 128, 128), BF16),
            pltpu.VMEM((2048, 128), F32),
            pltpu.VMEM((8, 256, 128), BF16),
            pltpu.VMEM((32, 64, 128), BF16),
            pltpu.VMEM((16, 128), F32),
            dma((12,)),
            dma((2,)),
            dma((2, 4, 4, 2)),
            dma((2, 4, 4, 2)),
            dma((4, 4)),
            dma((4, 4)),
            dma((3, 4, 2)),
            dma((3, 4, 2)),
            dma((3,)),
            dma((3,)),
            dma((32,)),
            dma((32,)),
            dma((2,)),
        ],
        compiler_params=pltpu.CompilerParams(
            collective_id=0, has_side_effects=True, vmem_limit_bytes=56 * 1024 * 1024
        ),
        name="critic",
    )(
        tokens,
        norm_gain.reshape(16, 128),
        expert_ids.T,
        gate_codes.T,
        gate_weights,
        up_weights,
        down_weights,
        value_head,
    )
    values, targets = pl.pallas_call(
        last_kernel,
        out_shape=(jax.ShapeDtypeStruct((128, 128), F32), jax.ShapeDtypeStruct((1, 128), F32)),
        in_specs=[vmem] * 4,
        out_specs=(vmem, vmem),
        name="retrace",
    )(final, actions.reshape(1, -1), rewards.reshape(1, -1), trace_codes.reshape(1, -1))
    return values, targets.reshape(-1)


def solution(mesh):
    group, weight = P(("dp", "expert"), None), P("expert", ("dp", "tensor"), None)
    line = P(("dp", "expert"))
    in_specs = (
        P(("dp", "expert"), "tensor"),
        P(),
        group,
        group,
        weight,
        weight,
        weight,
        P(),
        line,
        line,
        line,
    )
    return jax.shard_map(
        per_device, mesh=mesh, in_specs=in_specs, out_specs=(group, line), check_vma=False
    )
```

```python
import functools

import jax
import jax.numpy as jnp
from jax import lax
from jax.experimental import pallas as pl
from jax.experimental.pallas import tpu as pltpu
from jax.sharding import PartitionSpec as P

DISCOUNT = 0.99
EPSILON = 1e-05
MESH = pl.DeviceIdType.MESH
F32, BF16 = jnp.float32, jnp.bfloat16

OFFSET = (0, 3, 1, 2)
SEEN_AS = (0, 2, 1, 3)
ROW_A = 48
WEIGHT_ROWS = ((0, 32), (32, 64), (96, 64), (160, 64))


def rows_by(a, b):
    return lax.dot_general(a, b, (((1,), (1,)), ((), ())), preferred_element_type=F32)


def silu(v):
    return v / (1.0 + jnp.exp(-v))


ORDER = (
    (
        (
            ("r", 1, 0, 0, 0), ("q", 1, 0, 0), ("w", 0), ("r", 0, 1, 0, 0), ("q", 0, 1, 0), ("r", 0, 2, 0, 1),
            ("r", 0, 0, 1, 0), ("r", 0, 0, 2, 1), ("f", 0, 0, 0), ("f", 0, 0, 1), ("w", "d"),
            ("r", 1, 0, 0, 1), ("p", 0), ("p", "d"), ("r", 0, 1, 0, 1), ("e", 1, 0), ("r", 0, 2, 0, 0),
            ("e", 2, 0), ("r", 0, 0, 1, 1), ("e", 0, 1), ("r", 0, 0, 2, 0), ("e", 0, 2), ("B", 0, 0),
            ("q", 0, 1, 1), ("r", 1, 1, 0, 0), ("r", 1, 2, 0, 0), ("r", 1, 0, 1, 0), ("r", 1, 0, 2, 0),
            ("B", 1, 0), ("q", 0, 2, 1), ("r", 0, 3, 0, 0), ("r", 0, 3, 0, 1), ("e", 3, 0), ("r", 0, 1, 1, 0),
            ("r", 0, 1, 2, 0), ("B", 2, 0), ("B", 0, 1), ("q", 0, 2, 0), ("r", 1, 1, 0, 1), ("r", 1, 2, 0, 1),
            ("r", 0, 0, 3, 1), ("r", 0, 0, 3, 0), ("e", 0, 3),
        ),
        ("A", 0),
    ),
    (
        (
            ("f", 0, 1, 0), ("B", 0, 2), ("r", 0, 1, 2, 1), ("e", 1, 2), ("f", 0, 1, 1), ("r", 1, 3, 0, 0),
            ("B", 3, 0), ("q", 0, 3, 0), ("w", 1), ("r", 0, 1, 1, 1), ("e", 1, 1), ("q", 0, 3, 1),
            ("r", 0, 2, 2, 1), ("r", 0, 2, 1, 1), ("B", 0, 3), ("r", 1, 3, 0, 1), ("p", 1), ("f", 0, 2, 1),
            ("f", 1, 0, 0), ("r", 0, 2, 1, 0), ("e", 2, 1), ("r", 0, 2, 2, 0), ("e", 2, 2), ("B", 1, 2),
            ("f", 0, 2, 0), ("r", 0, 1, 3, 0), ("r", 0, 1, 3, 1), ("e", 1, 3),
        ),
        ("B", 1),
    ),
    (
        (
            ("q", 1, 0, 1), ("B", 1, 1), ("r", 0, 3, 1, 0), ("r", 0, 3, 2, 0),
        ),
        ("I", 0),
    ),
    (
        (
            ("f", 0, 3, 0), ("B", 2, 1), ("r", 0, 3, 1, 1), ("e", 3, 1), ("r", 0, 3, 2, 1), ("e", 3, 2),
            ("f", 0, 3, 1), ("q", 1, 1, 0), ("B", 2, 2), ("r", 1, 0, 3, 0), ("r", 0, 2, 3, 1), ("q", 1, 1, 1),
            ("B", 1, 3), ("r", 0, 2, 3, 0), ("e", 2, 3), ("r", 1, 0, 2, 1), ("f", 1, 0, 1),
        ),
        ("B", 2),
    ),
    (
        (
            ("q", 1, 2, 0), ("q", 1, 2, 1), ("r", 1, 0, 1, 1), ("B", 3, 1), ("r", 0, 3, 3, 1), ("w", 2),
            ("q", 1, 3, 0), ("r", 0, 3, 3, 0), ("e", 3, 3), ("r", 1, 1, 2, 0),
        ),
        ("B", 3),
    ),
    (
        (
            ("q", 1, 3, 1), ("B", 3, 2), ("r", 1, 1, 1, 0), ("r", 1, 1, 2, 1), ("p", 2), ("f", 1, 1, 0),
            ("f", 1, 1, 1), ("B", 2, 3),
        ),
        ("F", 0),
    ),
    (
        (
            ("r", 1, 1, 1, 1), ("r", 1, 0, 3, 1),
        ),
        ("C", 4),
    ),
    (
        (
            ("r", 1, 2, 1, 0), ("f", 1, 2, 0), ("r", 1, 2, 2, 0), ("B", 3, 3), ("r", 1, 2, 1, 1),
            ("r", 1, 2, 2, 1), ("f", 1, 2, 1),
        ),
        ("F", 1),
    ),
    (
        (
            ("r", 1, 3, 1, 0), ("f", 1, 3, 0), ("r", 1, 3, 2, 0), ("r", 1, 3, 1, 1), ("r", 1, 3, 2, 1),
            ("f", 1, 3, 1), ("r", 1, 1, 3, 0), ("r", 1, 1, 3, 1),
        ),
        ("C", 5),
    ),
    (
        (
            ("r", 1, 2, 3, 0), ("r", 1, 2, 3, 1),
        ),
        ("C", 6),
    ),
    (
        (
            ("r", 1, 3, 3, 0), ("r", 1, 3, 3, 1), ("w", 3),
        ),
        ("C", 7),
    ),
    (
        (
            ("p", 3),
        ),
        ("G", 0),
    ),
    (
        (
        ),
        ("G", 1),
    ),
)


def pick(index, values):
    out = values[-1]
    for i in range(len(values) - 2, -1, -1):
        out = jnp.where(index == i, values[i], out)
    return out


def kernel(
    tokens_ref,
    gain_ref,
    ids_ref,
    codes_ref,
    gate_ref,
    up_ref,
    down_ref,
    head_ref,
    final_ref,
    tin,
    rin,
    tok,
    wb,
    down_v,
    head_v,
    folded,
    heads,
    acc,
    stage,
    parts,
    gain_v,
    local_sem,
    raw_sem,
    tok_recv,
    tok_send,
    b_recv,
    b_send,
    w_recv,
    w_send,
    d_recv,
    d_send,
    rs_recv,
    rs_send,
    fin_sem,
):
    dp, z, c = lax.axis_index("dp"), lax.axis_index("expert"), lax.axis_index("tensor")
    x, y = dp % 4, dp // 4
    x_one = x + 1 - 2 * (x % 2)
    x_two = (x + 2 * (x % 2) + 3) % 4
    first, second = y * (1 - c) + z * c, z * (1 - c) + y * c

    def device(x_, f_, s_):
        y_, z_ = f_ * (1 - c) + s_ * c, s_ * (1 - c) + f_ * c
        return (y_ * 4 + x_, z_, c)

    partner = (dp, z, 1 - c)
    other = (y * 4 + x_one, z, c)
    twin = device(x_two, first, second)
    f_next = device(x, (first + 1) % 4, second)
    f_prev = device(x, (first + 3) % 4, second)
    s_next = device(x, first, (second + 1) % 4)
    s_prev = device(x, first, (second + 3) % 4)

    def remote(src, dst, send, recv, to):
        return pltpu.make_async_remote_copy(
            src_ref=src, dst_ref=dst, send_sem=send, recv_sem=recv, device_id=to, device_id_type=MESH
        )

    loads = [pltpu.make_async_copy(tokens_ref.at[pl.ds(i * 64, 64)], tin.at[i], local_sem.at[i]) for i in range(2)]
    w_loads = []
    for n, (at, size) in enumerate(WEIGHT_ROWS):
        chunk = n - 1 if n else 3
        for i, ref in enumerate((gate_ref, up_ref)):
            w_loads.append(
                pltpu.make_async_copy(
                    ref.at[0, pl.ds(at, size)], wb.at[chunk, pl.ds(i * 128, size)], local_sem.at[2 + 2 * n + i]
                )
            )
    d_loads = [
        pltpu.make_async_copy(down_ref.at[0], down_v, local_sem.at[10]),
        pltpu.make_async_copy(head_ref, head_v, local_sem.at[11]),
    ]
    for copy in loads + w_loads + d_loads:
        copy.start()

    barrier = pltpu.get_barrier_semaphore()
    for to in (partner, other, twin, f_next, f_prev, s_next, s_prev):
        pl.semaphore_signal(barrier, inc=1, device_id=to, device_id_type=MESH)
    for copy in loads:
        copy.wait()
    pl.semaphore_wait(barrier, 7)

    sends = []

    def start(make, *args):
        make(*args).start()
        sends.append((make, args))

    def raw_copy():
        return remote(tin.at[1 - c], rin, raw_sem.at[0], raw_sem.at[1], partner)

    start(raw_copy)
    for copy in w_loads:
        copy.wait()

    def weight_copy(n, i, role):
        size = WEIGHT_ROWS[n][1]
        mine, theirs = (n - 1, n + 3) if n else (3, 3)
        if role == 0:
            src, dst, at, to = mine, mine, (0, size), partner
        elif role == 1:
            src, dst, at, to = mine, theirs, (0, 0 if n else 2 * size), other
        else:
            src, dst, at, to = theirs, theirs, (0, size) if n else (2 * size, 3 * size), partner
        return remote(
            wb.at[src, pl.ds(i * 128 + at[0], size)],
            wb.at[dst, pl.ds(i * 128 + at[1], size)],
            w_send.at[role, n, i],
            w_recv.at[role, n, i],
            to,
        )

    for i in range(2):
        start(weight_copy, 0, i, 1)
    for n in range(4):
        for i in range(2):
            start(weight_copy, n, i, 0)

    raw_copy().wait_recv()
    mine = tin[c].astype(F32)
    theirs = rin[...].astype(F32)
    square = jnp.sum(mine * mine, axis=1, keepdims=True) + jnp.sum(theirs * theirs, axis=1, keepdims=True)
    scaling = lax.rsqrt(square / 2048.0 + EPSILON)
    gain_v[...] = gain_ref[...].astype(F32)
    for part, at in ((mine, c), (theirs, 1 - c)):
        for i in range(8):
            lanes = pl.ds(pl.multiple_of(at * 1024 + 128 * i, 128), 128)
            gain = gain_v[pl.ds(8 * at + i, 1), :]
            tok[0, pl.ds(0, 64), lanes] = (part[:, 128 * i : 128 * i + 128] * scaling * gain).astype(BF16)

    def block(g, l, s, h):
        return tok.at[4 * g + l, pl.ds(64 * s, 64 if g == 0 else ROW_A), pl.ds(1024 * h, 1024)]

    def token_copy(g, src, dst, h, to):
        return remote(
            block(g, *src, h), block(g, *dst, h), tok_send.at[g, *dst, h], tok_recv.at[g, *dst, h], to
        )

    def along_second(g, l, h):
        start(token_copy, g, (l, 0), (l, 1), h, s_next)
        start(token_copy, g, (l, 0), (l, 2), h, s_prev)

    def along_first(g, h, up):
        if up:
            start(token_copy, g, (0, 0), (1, 0), h, f_next)
        else:
            start(token_copy, g, (0, 0), (2, 0), h, f_prev)

    def edge(ref, l, s):
        return ref.at[l, pl.ds(64 * s + ROW_A, 64 - ROW_A)]

    def edge_copy(l, s):
        return remote(edge(tok, l, s), edge(tok, 4 + l, s), b_send.at[l, s], b_recv.at[l, s], twin)

    def twin_copy(h):
        src = tok.at[0, pl.ds(0, ROW_A), pl.ds(1024 * h, 1024)]
        return remote(src, block(1, 0, 0, h), tok_send.at[1, 0, 0, h], tok_recv.at[1, 0, 0, h], twin)

    for h in range(2):
        along_first(0, h, True)
        along_first(0, 1 - h, False)
        start(twin_copy, h)
        start(token_copy, 0, (0, 0), (0, 1), h, s_next)
        start(token_copy, 0, (0, 0), (0, 2), 1 - h, s_prev)
    start(edge_copy, 0, 0)

    for copy in d_loads:
        copy.wait()
    folded[0] = jnp.dot(down_v[...], head_v[...], preferred_element_type=F32).astype(BF16)

    def head_copy(role):
        src, dst, to = ((0, 1, partner), (0, 2, other), (2, 3, partner))[role]
        return remote(folded.at[src], folded.at[dst], d_send.at[role], d_recv.at[role], to)

    start(head_copy, 1)
    start(head_copy, 0)
    for n in range(1, 4):
        for i in range(2):
            start(weight_copy, n, i, 1)

    def happen(event):
        kind = event[0]
        if kind == "r":
            _, g, l, s, h = event
            token_copy(g, (l, s), (l, s), h, partner).wait_recv()
            if s == 0:
                if l == 0:
                    along_first(g, h, True)
                    along_first(g, h, False)
                if (l, h) == (1, 0):
                    start(token_copy, g, (1, 0), (3, 0), 0, f_next)
                if (l, h) == (2, 1):
                    start(token_copy, g, (2, 0), (3, 0), 1, f_prev)
        elif kind == "q":
            along_second(*event[1:])
        elif kind == "f":
            _, g, l, h = event
            start(token_copy, g, (l, 1 + h), (l, 3), h, s_prev if h else s_next)
        elif kind == "e":
            start(edge_copy, event[1], event[2])
        elif kind == "B":
            edge_copy(event[1], event[2]).wait_recv()
        elif kind == "w":
            if event[1] == "d":
                head_copy(1).wait_recv()
                start(head_copy, 2)
            else:
                for i in range(2):
                    weight_copy(event[1], i, 1).wait_recv()
                    start(weight_copy, event[1], i, 2)
        elif event[1] != "d":
            for i in range(2):
                weight_copy(event[1], i, 2).wait_recv()
        else:
            head_copy(0).wait_recv()
            head_copy(2).wait_recv()
            for n in range(4):
                at, size = WEIGHT_ROWS[n]
                for j in range(4):
                    if n == 0:
                        heads[3, pl.ds(32 * j, 32)] = folded[j, pl.ds(at, size)]
                    else:
                        heads[n - 1 + 4 * (j // 2), pl.ds(64 * (j % 2), 64)] = folded[j, pl.ds(at, size)]

    for n in range(4):
        for i in range(2):
            weight_copy(n, i, 0).wait_recv()

    def gated(product, count):
        hidden = [
            (silu(product[:, 256 * k : 256 * k + 128]) * product[:, 256 * k + 128 : 256 * k + 256]).astype(BF16)
            for k in range(count)
        ]
        return jnp.concatenate(hidden, axis=1) if count > 1 else hidden[0]

    def unit(b, size, low, high):
        if high is None:
            count, weights, head = 1, wb[low], heads[low]
        else:
            count = high - low
            weights = wb[low:high].reshape(256 * count, 2048)
            head = heads[low:high].reshape(128 * count, 128)
        product = rows_by(tok[pl.ds(size * b, size)].reshape(256 * size, 2048), weights)
        value = jnp.dot(gated(product, count), head, preferred_element_type=F32)
        rows = pl.ds(pl.multiple_of(256 * size * b, 256), 256 * size)
        if high is not None and low == 0:
            acc[rows] = value
        else:
            acc[rows] += value

    def part_copy(p, r, s):
        g, q = p // 2, p % 2
        to = device(
            x + g * (x_two - x), (first + q + r * (3 - 2 * q)) % 4, (second + OFFSET[s]) % 4
        )
        src = stage.at[2 * p + r, pl.ds(64 * s, 64)]
        slot = g * 16 + (q + 2 * r) * 4 + SEEN_AS[s]
        return remote(src, parts.at[slot], rs_send.at[slot], rs_recv.at[slot], to)

    def step(u, _):
        for i, (events, _) in enumerate(ORDER):
            if events:

                @pl.when(u == i)
                def _():
                    for event in events:
                        happen(event)

        kind = pick(u, ["ABCDHIEFG".index(work[0]) for _, work in ORDER])
        b = pick(u, [work[1] for _, work in ORDER])
        for i, (low, high) in enumerate(((0, 4), (0, 5), (0, 6), (4, 6), (5, 6), (4, 5))):

            @pl.when(kind == i)
            def _():
                unit(b, 1, low, high)

        @pl.when((kind == 6) | (kind == 7))
        def _():
            unit(b, 2, kind - 2, None)

        @pl.when(kind == 8)
        def _():
            products = [rows_by(tok[pl.ds(4 * b + 2 * i, 2)].reshape(512, 2048), wb[6]) for i in range(2)]
            for i in range(2):
                rows = pl.ds(pl.multiple_of(1024 * b + 512 * i, 512), 512)
                total = acc[rows] + jnp.dot(gated(products[i], 1), heads[6], preferred_element_type=F32)
                stage[pl.ds(4 * b + 2 * i, 2)] = total.astype(BF16).reshape(2, 256, 128)
                if i == 0:

                    @pl.when(b == 0)
                    def _():
                        acc[0:64] = total[0:64]

                for r in range(2):
                    for s in range(4):
                        if (i, r, s) == (0, 0, 0):

                            @pl.when(b > 0)
                            def _():
                                part_copy(2 * b, 0, 0).start()

                        else:
                            part_copy(2 * b + i, r, s).start()

        return 0

    lax.fori_loop(0, len(ORDER), step, 0)

    spot = lax.broadcasted_iota(jnp.int32, (64, 128), 1) == lax.broadcasted_iota(jnp.int32, (64, 128), 0) + 64 * c

    def upright(ref, i):
        return jnp.sum(jnp.where(spot, ref[i : i + 1, :], 0), axis=1, keepdims=True)

    ids = [upright(ids_ref, i) for i in range(2)]
    codes = [upright(codes_ref, i).astype(F32) for i in range(2)]
    share = [code / (codes[0] + codes[1]) for code in codes]
    shares = []
    for j in range(4):
        e = (z + OFFSET[j]) % 4
        shares.append(jnp.where(ids[0] == e, share[0], 0.0) + jnp.where(ids[1] == e, share[1], 0.0))
    c_wide = c.astype(F32)

    for slot in range(1, 32):
        remote(parts.at[slot], parts.at[slot], rs_send.at[slot], rs_recv.at[slot], partner).wait_recv()
    blended = jnp.zeros((64, 128), F32)
    for l in range(4):
        for s in range(4):
            slot = 4 * l + s
            near = parts[slot].astype(F32) if slot else acc[0:64]
            weight = shares[s] * (1.0 - c_wide) + shares[l] * c_wide
            blended += (near + parts[16 + slot].astype(F32)) * weight
    rows = pl.ds(pl.multiple_of(64 * c, 64), 64)
    final_ref[rows] = blended

    def final_copy():
        return remote(final_ref.at[rows], final_ref.at[rows], fin_sem.at[0], fin_sem.at[1], partner)

    start(final_copy)
    final_copy().wait_recv()

    for make, args in sends:
        make(*args).wait_send()
    for slot in range(1, 32):
        remote(parts.at[slot], parts.at[slot], rs_send.at[slot], rs_recv.at[slot], partner).wait_send()


def last_kernel(final_ref, actions_ref, rewards_ref, trace_ref, values_ref, targets_ref):
    values = final_ref[...]
    values_ref[...] = values
    lane = lax.broadcasted_iota(jnp.int32, (128, 128), 1)
    row = lax.broadcasted_iota(jnp.int32, (128, 128), 0)

    def column(v):
        return jnp.sum(jnp.where(lane == row, v, 0.0), axis=1, keepdims=True)

    trace = trace_ref[...].astype(F32) / 1024.0
    reward = rewards_ref[...].astype(F32) * 0.25
    action_column = jnp.sum(jnp.where(lane == row, actions_ref[...], 0), axis=1, keepdims=True)
    greedy = jnp.max(values, axis=1, keepdims=True)
    taken = jnp.sum(jnp.where(lane == action_column, values, 0.0), axis=1, keepdims=True)
    ahead = greedy - column(trace) * taken
    driver = reward + DISCOUNT * jnp.sum(jnp.where(row == lane + 1, ahead, 0.0), axis=0, keepdims=True)
    logs = jnp.log(DISCOUNT * trace)
    sums_column = jnp.sum(jnp.where(lane <= row, logs, 0.0), axis=1, keepdims=True)
    sums_row = jnp.sum(jnp.where(lane == row, sums_column, 0.0), axis=0, keepdims=True)
    weight = jnp.where(lane >= row, jnp.exp(jnp.minimum(sums_row - sums_column, 0.0)), 0.0)
    target = jnp.sum(weight * driver, axis=1, keepdims=True)
    targets_ref[...] = jnp.sum(jnp.where(lane == row, target, 0.0), axis=0, keepdims=True)


def per_device(
    tokens,
    norm_gain,
    expert_ids,
    gate_codes,
    gate_weights,
    up_weights,
    down_weights,
    value_head,
    actions,
    rewards,
    trace_codes,
):
    dma = pltpu.SemaphoreType.DMA
    vmem, hbm = pl.BlockSpec(memory_space=pltpu.VMEM), pl.BlockSpec(memory_space=pl.ANY)
    final = pl.pallas_call(
        kernel,
        out_shape=jax.ShapeDtypeStruct((128, 128), F32),
        in_specs=[hbm, vmem, vmem, vmem, hbm, hbm, hbm, hbm],
        out_specs=vmem,
        scratch_shapes=[
            pltpu.VMEM((2, 64, 1024), BF16),
            pltpu.VMEM((64, 1024), BF16),
            pltpu.VMEM((8, 256, 2048), BF16),
            pltpu.VMEM((7, 256, 2048), BF16),
            pltpu.VMEM((224, 2048), BF16),
            pltpu.VMEM((2048, 128), BF16),
            pltpu.VMEM((4, 224, 128), BF16),
            pltpu.VMEM((7, 128, 128), BF16),
            pltpu.VMEM((2048, 128), F32),
            pltpu.VMEM((8, 256, 128), BF16),
            pltpu.VMEM((32, 64, 128), BF16),
            pltpu.VMEM((16, 128), F32),
            dma((12,)),
            dma((2,)),
            dma((2, 4, 4, 2)),
            dma((2, 4, 4, 2)),
            dma((4, 4)),
            dma((4, 4)),
            dma((3, 4, 2)),
            dma((3, 4, 2)),
            dma((3,)),
            dma((3,)),
            dma((32,)),
            dma((32,)),
            dma((2,)),
        ],
        compiler_params=pltpu.CompilerParams(
            collective_id=0, has_side_effects=True, vmem_limit_bytes=56 * 1024 * 1024
        ),
        name="critic",
    )(
        tokens,
        norm_gain.reshape(16, 128),
        expert_ids.T,
        gate_codes.T,
        gate_weights,
        up_weights,
        down_weights,
        value_head,
    )
    values, targets = pl.pallas_call(
        last_kernel,
        out_shape=(jax.ShapeDtypeStruct((128, 128), F32), jax.ShapeDtypeStruct((1, 128), F32)),
        in_specs=[vmem] * 4,
        out_specs=(vmem, vmem),
        name="retrace",
    )(final, actions.reshape(1, -1), rewards.reshape(1, -1), trace_codes.reshape(1, -1))
    return values, targets.reshape(-1)


def solution(mesh):
    group, weight = P(("dp", "expert"), None), P("expert", ("dp", "tensor"), None)
    line = P(("dp", "expert"))
    in_specs = (
        P(("dp", "expert"), "tensor"),
        P(),
        group,
        group,
        weight,
        weight,
        weight,
        P(),
        line,
        line,
        line,
    )
    return jax.shard_map(
        per_device, mesh=mesh, in_specs=in_specs, out_specs=(group, line), check_vma=False
    )
```

```python
import functools

import jax
import jax.numpy as jnp
from jax import lax
from jax.experimental import pallas as pl
from jax.experimental.pallas import tpu as pltpu
from jax.sharding import PartitionSpec as P

DISCOUNT = 0.99
EPSILON = 1e-05
MESH = pl.DeviceIdType.MESH
F32, BF16 = jnp.float32, jnp.bfloat16

OFFSET = (0, 3, 1, 2)
SEEN_AS = (0, 2, 1, 3)
ROW_A = 48
WEIGHT_ROWS = ((0, 32), (32, 64), (96, 64), (160, 64))


def rows_by(a, b):
    return lax.dot_general(a, b, (((1,), (1,)), ((), ())), preferred_element_type=F32)


def silu(v):
    return v / (1.0 + jnp.exp(-v))


ORDER = (
    (
        (
            ("r", 1, 0, 0, 0), ("q", 1, 0, 0), ("w", 0), ("r", 0, 1, 0, 0), ("q", 0, 1, 0), ("r", 0, 2, 0, 1),
            ("r", 0, 0, 1, 0), ("r", 0, 0, 2, 1), ("f", 0, 0, 0), ("f", 0, 0, 1), ("w", "d"),
            ("r", 1, 0, 0, 1), ("p", 0), ("p", "d"), ("r", 0, 1, 0, 1), ("e", 1, 0), ("r", 0, 2, 0, 0),
            ("e", 2, 0), ("r", 0, 0, 1, 1), ("e", 0, 1), ("r", 0, 0, 2, 0), ("e", 0, 2), ("B", 0, 0),
            ("q", 0, 1, 1), ("r", 1, 1, 0, 0), ("r", 1, 2, 0, 0), ("r", 1, 0, 1, 0), ("r", 1, 0, 2, 0),
            ("B", 1, 0), ("q", 0, 2, 1), ("r", 0, 3, 0, 0), ("r", 0, 3, 0, 1), ("e", 3, 0), ("r", 0, 1, 1, 0),
            ("r", 0, 1, 2, 0),
        ),
        ("A", 0),
    ),
    (
        (
            ("B", 2, 0), ("B", 0, 1), ("q", 0, 2, 0), ("r", 1, 1, 0, 1), ("r", 1, 2, 0, 1), ("r", 0, 0, 3, 1),
            ("r", 0, 0, 3, 0), ("e", 0, 3), ("B", 0, 2), ("f", 0, 1, 0), ("r", 0, 1, 2, 1), ("e", 1, 2),
            ("f", 0, 1, 1), ("r", 1, 3, 0, 0), ("B", 3, 0), ("q", 0, 3, 0), ("w", 1), ("r", 0, 1, 1, 1),
            ("e", 1, 1),
        ),
        ("A", 1),
    ),
    (
        (
            ("q", 0, 3, 1), ("r", 0, 2, 2, 1), ("r", 0, 2, 1, 1), ("B", 0, 3), ("r", 1, 3, 0, 1),
        ),
        ("A", 4),
    ),
    (
        (
            ("f", 0, 2, 1), ("f", 1, 0, 0), ("p", 1), ("r", 0, 2, 1, 0), ("e", 2, 1), ("r", 0, 2, 2, 0),
            ("e", 2, 2), ("B", 1, 2),
        ),
        ("E", 0),
    ),
    (
        (
            ("f", 0, 2, 0), ("r", 0, 1, 3, 0), ("r", 0, 1, 3, 1), ("e", 1, 3), ("B", 1, 1), ("q", 1, 0, 1),
            ("r", 0, 3, 1, 0), ("r", 0, 3, 2, 0), ("f", 0, 3, 0), ("B", 2, 1), ("r", 0, 3, 1, 1), ("e", 3, 1),
            ("r", 0, 3, 2, 1), ("e", 3, 2), ("f", 0, 3, 1),
        ),
        ("B", 2),
    ),
    (
        (
            ("q", 1, 1, 0), ("q", 1, 1, 1), ("r", 1, 0, 3, 0), ("B", 2, 2), ("r", 0, 2, 3, 1),
            ("r", 0, 2, 3, 0), ("e", 2, 3), ("r", 1, 0, 2, 1), ("f", 1, 0, 1), ("B", 1, 3), ("q", 1, 2, 0),
            ("r", 1, 0, 1, 1), ("q", 1, 2, 1), ("r", 0, 3, 3, 1), ("w", 2), ("B", 3, 1), ("q", 1, 3, 0),
            ("r", 0, 3, 3, 0), ("e", 3, 3),
        ),
        ("B", 3),
    ),
    (
        (
            ("q", 1, 3, 1), ("r", 1, 1, 2, 0), ("B", 3, 2), ("p", 2), ("r", 1, 1, 1, 0), ("r", 1, 1, 2, 1),
            ("f", 1, 1, 0),
        ),
        ("F", 0),
    ),
    (
        (
            ("f", 1, 1, 1), ("B", 2, 3), ("r", 1, 1, 1, 1), ("r", 1, 0, 3, 1),
        ),
        ("C", 5),
    ),
    (
        (
            ("r", 1, 2, 1, 0), ("f", 1, 2, 0), ("r", 1, 2, 2, 0), ("B", 3, 3), ("r", 1, 2, 1, 1),
            ("r", 1, 2, 2, 1), ("f", 1, 2, 1),
        ),
        ("F", 1),
    ),
    (
        (
            ("r", 1, 3, 1, 0), ("f", 1, 3, 0), ("r", 1, 3, 2, 0),
        ),
        ("D", 4),
    ),
    (
        (
            ("r", 1, 3, 1, 1), ("r", 1, 3, 2, 1), ("f", 1, 3, 1),
        ),
        ("C", 6),
    ),
    (
        (
            ("r", 1, 1, 3, 0), ("r", 1, 1, 3, 1), ("r", 1, 2, 3, 0), ("r", 1, 2, 3, 1), ("r", 1, 3, 3, 0),
            ("r", 1, 3, 3, 1), ("w", 3),
        ),
        ("C", 7),
    ),
    (
        (
            ("p", 3),
        ),
        ("G", 0),
    ),
)


BLOCKS = (
    ((0, 0), (1, 0), (2, 0), (3, 0)),
    ((0, 1), (0, 2), (1, 1), (1, 2)),
    ((2, 1), (2, 2), (3, 1), (3, 2)),
    ((0, 3), (1, 3), (2, 3), (3, 3)),
)
PLACE = {block: (i, j) for i, blocks in enumerate(BLOCKS) for j, block in enumerate(blocks)}


def pick(index, values):
    out = values[-1]
    for i in range(len(values) - 2, -1, -1):
        out = jnp.where(index == i, values[i], out)
    return out


def kernel(
    tokens_ref,
    gain_hbm,
    ids_hbm,
    codes_hbm,
    gate_ref,
    up_ref,
    down_ref,
    head_ref,
    final_ref,
    gain_ref,
    ids_ref,
    codes_ref,
    tin,
    rin,
    tok,
    wb,
    down_v,
    head_v,
    folded,
    heads,
    acc,
    stage,
    parts,
    gain_v,
    local_sem,
    raw_sem,
    tok_recv,
    tok_send,
    b_recv,
    b_send,
    w_recv,
    w_send,
    d_recv,
    d_send,
    rs_recv,
    rs_send,
    fin_sem,
):
    dp, z, c = lax.axis_index("dp"), lax.axis_index("expert"), lax.axis_index("tensor")
    x, y = dp % 4, dp // 4
    x_one = x + 1 - 2 * (x % 2)
    x_two = (x + 2 * (x % 2) + 3) % 4
    first, second = y * (1 - c) + z * c, z * (1 - c) + y * c

    def device(x_, f_, s_):
        y_, z_ = f_ * (1 - c) + s_ * c, s_ * (1 - c) + f_ * c
        return (y_ * 4 + x_, z_, c)

    partner = (dp, z, 1 - c)
    other = (y * 4 + x_one, z, c)
    twin = device(x_two, first, second)
    f_next = device(x, (first + 1) % 4, second)
    f_prev = device(x, (first + 3) % 4, second)
    s_next = device(x, first, (second + 1) % 4)
    s_prev = device(x, first, (second + 3) % 4)

    def remote(src, dst, send, recv, to):
        return pltpu.make_async_remote_copy(
            src_ref=src, dst_ref=dst, send_sem=send, recv_sem=recv, device_id=to, device_id_type=MESH
        )

    barrier = pltpu.get_barrier_semaphore()
    for to in (partner, other, twin, f_next, f_prev, s_next, s_prev):
        pl.semaphore_signal(barrier, inc=1, device_id=to, device_id_type=MESH)
    loads = [pltpu.make_async_copy(tokens_ref.at[pl.ds(i * 64, 64)], tin.at[i], local_sem.at[i]) for i in range(2)]
    w_loads = []
    for n, (at, size) in enumerate(WEIGHT_ROWS):
        chunk = n - 1 if n else 3
        for i, ref in enumerate((gate_ref, up_ref)):
            w_loads.append(
                pltpu.make_async_copy(
                    ref.at[0, pl.ds(at, size)], wb.at[chunk, pl.ds(i * 128, size)], local_sem.at[2 + 2 * n + i]
                )
            )
    d_loads = [
        pltpu.make_async_copy(down_ref.at[0], down_v, local_sem.at[10]),
        pltpu.make_async_copy(head_ref, head_v, local_sem.at[11]),
    ]
    small = [
        pltpu.make_async_copy(src, dst, local_sem.at[12 + i])
        for i, (src, dst) in enumerate(((gain_hbm, gain_ref), (ids_hbm, ids_ref), (codes_hbm, codes_ref)))
    ]
    for copy in loads + w_loads[:2] + small[:1] + w_loads[2:] + d_loads + small[1:]:
        copy.start()

    for copy in loads:
        copy.wait()
    pl.semaphore_wait(barrier, 7)

    sends = []

    def start(make, *args):
        make(*args).start()
        sends.append((make, args))

    def raw_copy():
        return remote(tin.at[1 - c], rin, raw_sem.at[0], raw_sem.at[1], partner)

    start(raw_copy)
    for copy in w_loads[:2]:
        copy.wait()

    def weight_copy(n, i, role):
        size = WEIGHT_ROWS[n][1]
        mine, theirs = (n - 1, n + 3) if n else (3, 3)
        if role == 0:
            src, dst, at, to = mine, mine, (0, size), partner
        elif role == 1:
            src, dst, at, to = mine, theirs, (0, 0 if n else 2 * size), other
        else:
            src, dst, at, to = theirs, theirs, (0, size) if n else (2 * size, 3 * size), partner
        return remote(
            wb.at[src, pl.ds(i * 128 + at[0], size)],
            wb.at[dst, pl.ds(i * 128 + at[1], size)],
            w_send.at[role, n, i],
            w_recv.at[role, n, i],
            to,
        )

    for i in range(2):
        start(weight_copy, 0, i, 1)
    for copy in small:
        copy.wait()
    for copy in w_loads[2:]:
        copy.wait()
    for n in range(4):
        for i in range(2):
            start(weight_copy, n, i, 0)

    raw_copy().wait_recv()
    mine = tin[c].astype(F32)
    theirs = rin[...].astype(F32)
    square = jnp.sum(mine * mine, axis=1, keepdims=True) + jnp.sum(theirs * theirs, axis=1, keepdims=True)
    scaling = lax.rsqrt(square / 2048.0 + EPSILON)
    gain_v[...] = gain_ref[...].astype(F32)
    for part, at in ((mine, c), (theirs, 1 - c)):
        for i in range(8):
            lanes = pl.ds(pl.multiple_of(at * 1024 + 128 * i, 128), 128)
            gain = gain_v[pl.ds(8 * at + i, 1), :]
            tok[0, pl.ds(0, 64), lanes] = (part[:, 128 * i : 128 * i + 128] * scaling * gain).astype(BF16)

    def block(g, l, s, h):
        i, j = PLACE[l, s]
        return tok.at[4 * g + i, pl.ds(64 * j, 64 if g == 0 else ROW_A), pl.ds(1024 * h, 1024)]

    def token_copy(g, src, dst, h, to):
        return remote(
            block(g, *src, h), block(g, *dst, h), tok_send.at[g, *dst, h], tok_recv.at[g, *dst, h], to
        )

    def along_second(g, l, h):
        start(token_copy, g, (l, 0), (l, 1), h, s_next)
        start(token_copy, g, (l, 0), (l, 2), h, s_prev)

    def along_first(g, h, up):
        if up:
            start(token_copy, g, (0, 0), (1, 0), h, f_next)
        else:
            start(token_copy, g, (0, 0), (2, 0), h, f_prev)

    def edge(g, l, s):
        i, j = PLACE[l, s]
        return tok.at[4 * g + i, pl.ds(64 * j + ROW_A, 64 - ROW_A)]

    def edge_copy(l, s):
        return remote(edge(0, l, s), edge(1, l, s), b_send.at[l, s], b_recv.at[l, s], twin)

    def twin_copy(h):
        src = tok.at[0, pl.ds(0, ROW_A), pl.ds(1024 * h, 1024)]
        return remote(src, block(1, 0, 0, h), tok_send.at[1, 0, 0, h], tok_recv.at[1, 0, 0, h], twin)

    for h in range(2):
        along_first(0, h, True)
        along_first(0, 1 - h, False)
        start(twin_copy, h)
        start(token_copy, 0, (0, 0), (0, 1), h, s_next)
        start(token_copy, 0, (0, 0), (0, 2), 1 - h, s_prev)
    start(edge_copy, 0, 0)

    for copy in d_loads:
        copy.wait()
    folded[0] = jnp.dot(down_v[...], head_v[...], preferred_element_type=F32).astype(BF16)

    def head_copy(role):
        src, dst, to = ((0, 1, partner), (0, 2, other), (2, 3, partner))[role]
        return remote(folded.at[src], folded.at[dst], d_send.at[role], d_recv.at[role], to)

    start(head_copy, 1)
    start(head_copy, 0)
    for n in range(1, 4):
        for i in range(2):
            start(weight_copy, n, i, 1)

    def happen(event):
        kind = event[0]
        if kind == "r":
            _, g, l, s, h = event
            token_copy(g, (l, s), (l, s), h, partner).wait_recv()
            if s == 0:
                if l == 0:
                    along_first(g, h, True)
                    along_first(g, h, False)
                if (l, h) == (1, 0):
                    start(token_copy, g, (1, 0), (3, 0), 0, f_next)
                if (l, h) == (2, 1):
                    start(token_copy, g, (2, 0), (3, 0), 1, f_prev)
        elif kind == "q":
            along_second(*event[1:])
        elif kind == "f":
            _, g, l, h = event
            start(token_copy, g, (l, 1 + h), (l, 3), h, s_prev if h else s_next)
        elif kind == "e":
            start(edge_copy, event[1], event[2])
        elif kind == "B":
            edge_copy(event[1], event[2]).wait_recv()
        elif kind == "w":
            if event[1] == "d":
                head_copy(1).wait_recv()
                start(head_copy, 2)
            else:
                for i in range(2):
                    weight_copy(event[1], i, 1).wait_recv()
                    start(weight_copy, event[1], i, 2)
        elif event[1] != "d":
            for i in range(2):
                weight_copy(event[1], i, 2).wait_recv()
        else:
            head_copy(0).wait_recv()
            head_copy(2).wait_recv()
            for n in range(4):
                at, size = WEIGHT_ROWS[n]
                for j in range(4):
                    if n == 0:
                        heads[3, pl.ds(32 * j, 32)] = folded[j, pl.ds(at, size)]
                    else:
                        heads[n - 1 + 4 * (j // 2), pl.ds(64 * (j % 2), 64)] = folded[j, pl.ds(at, size)]

    for n in range(4):
        for i in range(2):
            weight_copy(n, i, 0).wait_recv()

    def gated(product, count):
        hidden = [
            (silu(product[:, 256 * k : 256 * k + 128]) * product[:, 256 * k + 128 : 256 * k + 256]).astype(BF16)
            for k in range(count)
        ]
        return jnp.concatenate(hidden, axis=1) if count > 1 else hidden[0]

    def unit(b, size, low, high):
        if high is None:
            count, weights, head = 1, wb[low], heads[low]
        else:
            count = high - low
            weights = wb[low:high].reshape(256 * count, 2048)
            head = heads[low:high].reshape(128 * count, 128)
        product = rows_by(tok[pl.ds(size * b, size)].reshape(256 * size, 2048), weights)
        value = jnp.dot(gated(product, count), head, preferred_element_type=F32)
        rows = pl.ds(pl.multiple_of(256 * size * b, 256), 256 * size)
        if high is not None and low == 0:
            acc[rows] = value
        else:
            acc[rows] += value

    def part_copy(g, l, s):
        to = device(x_two if g else x, (first + OFFSET[l]) % 4, (second + OFFSET[s]) % 4)
        i, j = PLACE[l, s]
        slot = 16 * g + 4 * SEEN_AS[l] + SEEN_AS[s]
        return remote(
            stage.at[4 * g + i, pl.ds(64 * j, 64)], parts.at[slot], rs_send.at[slot], rs_recv.at[slot], to
        )

    def finish(p, product):
        rows = pl.ds(512 * p, 512)
        total = acc[rows] + jnp.dot(gated(product, 1), heads[6], preferred_element_type=F32)
        stage[pl.ds(2 * p, 2)] = total.astype(BF16).reshape(2, 256, 128)
        for i in (2 * p + 1, 2 * p):
            for l, s in BLOCKS[i % 4]:
                if (i // 4, l, s) != (0, 0, 0):
                    part_copy(i // 4, l, s).start()
        if p == 0:
            acc[0:64] = total[0:64]

    def step(u, _):
        for i, (events, _) in enumerate(ORDER[:-1]):
            if events:

                @pl.when(u == i)
                def _():
                    for event in events:
                        happen(event)

        kind = pick(u, ["ABCDHIEFG".index(work[0]) for _, work in ORDER[:-1]])
        b = pick(u, [work[1] for _, work in ORDER[:-1]])
        for i, (low, high) in enumerate(((0, 4), (0, 5), (0, 6), (4, 6), (5, 6), (4, 5))):

            @pl.when(kind == i)
            def _():
                unit(b, 1, low, high)

        @pl.when((kind == 6) | (kind == 7))
        def _():
            unit(b, 2, kind - 2, None)

        return 0

    lax.fori_loop(0, len(ORDER) - 1, step, 0)

    for event in ORDER[-1][0]:
        happen(event)
    product = None
    for p in (3, 2, 1, 0):
        ahead = rows_by(tok[2 * p : 2 * p + 2].reshape(512, 2048), wb[6])
        if p < 3:
            finish(p + 1, product)
        product = ahead
    finish(0, product)

    spot = lax.broadcasted_iota(jnp.int32, (64, 128), 1) == lax.broadcasted_iota(jnp.int32, (64, 128), 0) + 64 * c

    def upright(ref, i):
        return jnp.sum(jnp.where(spot, ref[i : i + 1, :], 0), axis=1, keepdims=True)

    ids = [upright(ids_ref, i) for i in range(2)]
    codes = [upright(codes_ref, i).astype(F32) for i in range(2)]
    share = [code / (codes[0] + codes[1]) for code in codes]
    shares = []
    for j in range(4):
        e = (z + OFFSET[j]) % 4
        shares.append(jnp.where(ids[0] == e, share[0], 0.0) + jnp.where(ids[1] == e, share[1], 0.0))
    c_wide = c.astype(F32)

    def arrived(slot):
        remote(parts.at[slot], parts.at[slot], rs_send.at[slot], rs_recv.at[slot], partner).wait_recv()
        return parts[slot].astype(F32)

    blended = jnp.zeros((64, 128), F32)
    for s in (3, 2, 1, 0):
        for l in (3, 2, 1, 0):
            slot = 4 * l + s
            weight = shares[s] * (1.0 - c_wide) + shares[l] * c_wide
            far = arrived(16 + slot)
            near = arrived(slot) if slot else acc[0:64]
            blended += (near + far) * weight
    rows = pl.ds(pl.multiple_of(64 * c, 64), 64)
    final_ref[rows] = blended

    def final_copy():
        return remote(final_ref.at[rows], final_ref.at[rows], fin_sem.at[0], fin_sem.at[1], partner)

    start(final_copy)
    final_copy().wait_recv()

    for make, args in sends:
        make(*args).wait_send()
    for slot in range(1, 32):
        remote(parts.at[slot], parts.at[slot], rs_send.at[slot], rs_recv.at[slot], partner).wait_send()


def last_kernel(final_ref, actions_ref, rewards_ref, trace_ref, values_ref, targets_ref):
    values = final_ref[...]
    values_ref[...] = values
    lane = lax.broadcasted_iota(jnp.int32, (128, 128), 1)
    row = lax.broadcasted_iota(jnp.int32, (128, 128), 0)

    def column(v):
        return jnp.sum(jnp.where(lane == row, v, 0.0), axis=1, keepdims=True)

    trace = trace_ref[...].astype(F32) / 1024.0
    reward = rewards_ref[...].astype(F32) * 0.25
    action_column = jnp.sum(jnp.where(lane == row, actions_ref[...], 0), axis=1, keepdims=True)
    greedy = jnp.max(values, axis=1, keepdims=True)
    taken = jnp.sum(jnp.where(lane == action_column, values, 0.0), axis=1, keepdims=True)
    ahead = greedy - column(trace) * taken
    driver = reward + DISCOUNT * jnp.sum(jnp.where(row == lane + 1, ahead, 0.0), axis=0, keepdims=True)
    logs = jnp.log(DISCOUNT * trace)
    sums_column = jnp.sum(jnp.where(lane <= row, logs, 0.0), axis=1, keepdims=True)
    sums_row = jnp.sum(jnp.where(lane == row, sums_column, 0.0), axis=0, keepdims=True)
    weight = jnp.where(lane >= row, jnp.exp(jnp.minimum(sums_row - sums_column, 0.0)), 0.0)
    target = jnp.sum(weight * driver, axis=1, keepdims=True)
    targets_ref[...] = jnp.sum(jnp.where(lane == row, target, 0.0), axis=0, keepdims=True)


def per_device(
    tokens,
    norm_gain,
    expert_ids,
    gate_codes,
    gate_weights,
    up_weights,
    down_weights,
    value_head,
    actions,
    rewards,
    trace_codes,
):
    dma = pltpu.SemaphoreType.DMA
    vmem, hbm = pl.BlockSpec(memory_space=pltpu.VMEM), pl.BlockSpec(memory_space=pl.ANY)
    final = pl.pallas_call(
        kernel,
        out_shape=pltpu.VMEM((128, 128), F32),
        in_specs=[hbm] * 8,
        out_specs=vmem,
        scratch_shapes=[
            pltpu.VMEM((16, 128), BF16),
            pltpu.VMEM((2, 128), jnp.int32),
            pltpu.VMEM((2, 128), jnp.int32),
            pltpu.VMEM((2, 64, 1024), BF16),
            pltpu.VMEM((64, 1024), BF16),
            pltpu.VMEM((8, 256, 2048), BF16),
            pltpu.VMEM((7, 256, 2048), BF16),
            pltpu.VMEM((224, 2048), BF16),
            pltpu.VMEM((2048, 128), BF16),
            pltpu.VMEM((4, 224, 128), BF16),
            pltpu.VMEM((7, 128, 128), BF16),
            pltpu.VMEM((2048, 128), F32),
            pltpu.VMEM((8, 256, 128), BF16),
            pltpu.VMEM((32, 64, 128), BF16),
            pltpu.VMEM((16, 128), F32),
            dma((15,)),
            dma((2,)),
            dma((2, 4, 4, 2)),
            dma((2, 4, 4, 2)),
            dma((4, 4)),
            dma((4, 4)),
            dma((3, 4, 2)),
            dma((3, 4, 2)),
            dma((3,)),
            dma((3,)),
            dma((32,)),
            dma((32,)),
            dma((2,)),
        ],
        compiler_params=pltpu.CompilerParams(
            collective_id=0, has_side_effects=True, vmem_limit_bytes=56 * 1024 * 1024
        ),
        name="critic",
    )(
        tokens,
        norm_gain.reshape(16, 128),
        expert_ids.T,
        gate_codes.T,
        gate_weights,
        up_weights,
        down_weights,
        value_head,
    )
    values, targets = pl.pallas_call(
        last_kernel,
        out_shape=(jax.ShapeDtypeStruct((128, 128), F32), jax.ShapeDtypeStruct((1, 128), F32)),
        in_specs=[vmem] * 4,
        out_specs=(vmem, vmem),
        name="retrace",
    )(pltpu.with_memory_space_constraint(final, pltpu.VMEM), actions.reshape(1, -1), rewards.reshape(1, -1), trace_codes.reshape(1, -1))
    return values, targets.reshape(-1)


def solution(mesh):
    group, weight = P(("dp", "expert"), None), P("expert", ("dp", "tensor"), None)
    line = P(("dp", "expert"))
    in_specs = (
        P(("dp", "expert"), "tensor"),
        P(),
        group,
        group,
        weight,
        weight,
        weight,
        P(),
        line,
        line,
        line,
    )
    return jax.shard_map(
        per_device, mesh=mesh, in_specs=in_specs, out_specs=(group, line), check_vma=False
    )
```

```python
import functools

import jax
import jax.numpy as jnp
from jax import lax
from jax.experimental import pallas as pl
from jax.experimental.pallas import tpu as pltpu
from jax.sharding import PartitionSpec as P

DISCOUNT = 0.99
EPSILON = 1e-05
MESH = pl.DeviceIdType.MESH
F32, BF16 = jnp.float32, jnp.bfloat16

OFFSET = (0, 3, 1, 2)
SEEN_AS = (0, 2, 1, 3)
ROW_A = 48
WEIGHT_ROWS = ((0, 32), (32, 64), (96, 64), (160, 64))


def rows_by(a, b):
    return lax.dot_general(a, b, (((1,), (1,)), ((), ())), preferred_element_type=F32)


def silu(v):
    return v / (1.0 + jnp.exp(-v))


ORDER = (
    (
        (
            ("r", 1, 0, 0, 0), ("q", 1, 0, 0), ("r", 0, 1, 0, 0), ("q", 0, 1, 0), ("r", 0, 2, 0, 1),
            ("r", 0, 0, 1, 0), ("r", 0, 0, 2, 1), ("f", 0, 0, 0), ("f", 0, 0, 1), ("w", 0), ("r", 1, 0, 0, 1),
            ("w", "d"), ("p", 0), ("r", 0, 1, 0, 1), ("e", 1, 0), ("r", 0, 2, 0, 0), ("e", 2, 0),
            ("r", 0, 0, 1, 1), ("e", 0, 1), ("r", 0, 0, 2, 0), ("e", 0, 2), ("B", 0, 0), ("q", 0, 1, 1),
            ("p", "d"), ("r", 1, 1, 0, 0), ("r", 1, 2, 0, 0), ("r", 1, 0, 1, 0), ("r", 1, 0, 2, 0),
            ("q", 0, 2, 1), ("B", 1, 0), ("r", 0, 3, 0, 0), ("r", 0, 3, 0, 1), ("e", 3, 0), ("r", 0, 1, 1, 0),
            ("r", 0, 1, 2, 0),
        ),
        ("A", 0),
    ),
    (
        (
            ("f", 0, 1, 0), ("B", 2, 0), ("r", 1, 1, 0, 1), ("r", 1, 2, 0, 1), ("q", 0, 2, 0),
            ("r", 0, 0, 3, 1), ("B", 0, 1), ("r", 0, 0, 3, 0), ("e", 0, 3), ("q", 0, 3, 0), ("r", 0, 1, 2, 1),
            ("e", 1, 2), ("f", 0, 1, 1), ("B", 0, 2), ("r", 1, 3, 0, 0), ("r", 0, 1, 1, 1), ("e", 1, 1),
        ),
        ("A", 1),
    ),
    (
        (
            ("q", 0, 3, 1), ("r", 0, 2, 2, 1), ("B", 3, 0), ("w", 1), ("r", 0, 2, 1, 1), ("f", 0, 2, 1),
            ("f", 1, 0, 0), ("r", 1, 3, 0, 1),
        ),
        ("A", 4),
    ),
    (
        (
            ("q", 1, 0, 1), ("B", 0, 3), ("r", 0, 1, 3, 0), ("r", 0, 2, 2, 0), ("e", 2, 2), ("p", 1),
        ),
        ("E", 0),
    ),
    (
        (
            ("q", 1, 1, 0), ("B", 1, 2), ("r", 0, 2, 1, 0), ("e", 2, 1), ("f", 0, 2, 0), ("r", 0, 3, 2, 0),
            ("B", 1, 1), ("r", 0, 3, 1, 0), ("r", 0, 1, 3, 1), ("e", 1, 3), ("f", 0, 3, 0), ("r", 0, 3, 1, 1),
            ("e", 3, 1), ("r", 0, 3, 2, 1), ("e", 3, 2), ("f", 0, 3, 1),
        ),
        ("B", 2),
    ),
    (
        (
            ("q", 1, 1, 1), ("q", 1, 2, 0), ("r", 1, 0, 3, 0), ("r", 0, 2, 3, 1), ("B", 2, 2),
            ("r", 1, 0, 1, 1), ("r", 1, 0, 2, 1), ("f", 1, 0, 1), ("q", 1, 2, 1), ("B", 2, 1),
            ("r", 1, 1, 1, 0), ("r", 1, 1, 2, 0), ("f", 1, 1, 0), ("B", 1, 3), ("r", 0, 2, 3, 0), ("e", 2, 3),
            ("q", 1, 3, 0), ("w", 2), ("r", 0, 3, 3, 1), ("q", 1, 3, 1), ("B", 3, 1), ("r", 0, 3, 3, 0),
            ("e", 3, 3),
        ),
        ("B", 3),
    ),
    (
        (
            ("r", 1, 1, 2, 1), ("f", 1, 1, 1), ("p", 2), ("r", 1, 1, 1, 1), ("B", 3, 2), ("r", 1, 2, 2, 0),
        ),
        ("C", 5),
    ),
    (
        (
            ("r", 1, 2, 1, 0), ("f", 1, 2, 0), ("r", 1, 0, 3, 1), ("r", 1, 2, 1, 1), ("B", 2, 3),
            ("r", 1, 2, 2, 1), ("f", 1, 2, 1),
        ),
        ("F", 0),
    ),
    (
        (
            ("r", 1, 1, 3, 0), ("r", 1, 3, 2, 0), ("B", 3, 3),
        ),
        ("F", 1),
    ),
    (
        (
            ("r", 1, 3, 1, 0), ("f", 1, 3, 0), ("r", 1, 3, 2, 1), ("f", 1, 3, 1),
        ),
        ("D", 4),
    ),
    (
        (
            ("r", 1, 3, 1, 1), ("r", 1, 1, 3, 1),
        ),
        ("C", 6),
    ),
    (
        (
            ("r", 1, 2, 3, 0), ("r", 1, 2, 3, 1), ("w", 3), ("r", 1, 3, 3, 0), ("r", 1, 3, 3, 1),
        ),
        ("C", 7),
    ),
    (
        (
            ("p", 3),
        ),
        ("G", 0),
    ),
)

BLOCKS = (
    ((0, 0), (1, 0), (2, 0), (3, 0)),
    ((0, 1), (0, 2), (1, 1), (1, 2)),
    ((2, 1), (2, 2), (3, 1), (3, 2)),
    ((0, 3), (1, 3), (2, 3), (3, 3)),
)
PLACE = {block: (i, j) for i, blocks in enumerate(BLOCKS) for j, block in enumerate(blocks)}


def pick(index, values):
    out = values[-1]
    for i in range(len(values) - 2, -1, -1):
        out = jnp.where(index == i, values[i], out)
    return out


def kernel(
    tokens_ref,
    gain_hbm,
    ids_hbm,
    codes_hbm,
    gate_ref,
    up_ref,
    down_ref,
    head_ref,
    final_ref,
    gain_ref,
    ids_ref,
    codes_ref,
    tin,
    rin,
    tok,
    wb,
    down_v,
    head_v,
    folded,
    heads,
    acc,
    stage,
    parts,
    gain_v,
    local_sem,
    raw_sem,
    tok_recv,
    tok_send,
    b_recv,
    b_send,
    w_recv,
    w_send,
    d_recv,
    d_send,
    rs_recv,
    rs_send,
    fin_sem,
):
    dp, z, c = lax.axis_index("dp"), lax.axis_index("expert"), lax.axis_index("tensor")
    x, y = dp % 4, dp // 4
    x_one = x + 1 - 2 * (x % 2)
    x_two = (x + 2 * (x % 2) + 3) % 4
    first, second = y * (1 - c) + z * c, z * (1 - c) + y * c

    def device(x_, f_, s_):
        y_, z_ = f_ * (1 - c) + s_ * c, s_ * (1 - c) + f_ * c
        return (y_ * 4 + x_, z_, c)

    partner = (dp, z, 1 - c)
    other = (y * 4 + x_one, z, c)
    twin = device(x_two, first, second)
    f_next = device(x, (first + 1) % 4, second)
    f_prev = device(x, (first + 3) % 4, second)
    s_next = device(x, first, (second + 1) % 4)
    s_prev = device(x, first, (second + 3) % 4)

    def remote(src, dst, send, recv, to):
        return pltpu.make_async_remote_copy(
            src_ref=src, dst_ref=dst, send_sem=send, recv_sem=recv, device_id=to, device_id_type=MESH
        )

    barrier = pltpu.get_barrier_semaphore()
    for to in (partner, other, twin, f_next, f_prev, s_next, s_prev):
        pl.semaphore_signal(barrier, inc=1, device_id=to, device_id_type=MESH)
    loads = [pltpu.make_async_copy(tokens_ref.at[pl.ds(i * 64, 64)], tin.at[i], local_sem.at[i]) for i in range(2)]
    w_loads = []
    for n, (at, size) in enumerate(WEIGHT_ROWS):
        chunk = n - 1 if n else 3
        for i, ref in enumerate((gate_ref, up_ref)):
            w_loads.append(
                pltpu.make_async_copy(
                    ref.at[0, pl.ds(at, size)], wb.at[chunk, pl.ds(i * 128, size)], local_sem.at[2 + 2 * n + i]
                )
            )
    d_loads = [
        pltpu.make_async_copy(down_ref.at[0], down_v, local_sem.at[10]),
        pltpu.make_async_copy(head_ref, head_v, local_sem.at[11]),
    ]
    small = [
        pltpu.make_async_copy(src, dst, local_sem.at[12 + i])
        for i, (src, dst) in enumerate(((gain_hbm, gain_ref), (ids_hbm, ids_ref), (codes_hbm, codes_ref)))
    ]
    for copy in loads + w_loads[:2] + small[:1] + w_loads[2:] + d_loads + small[1:]:
        copy.start()

    for copy in loads:
        copy.wait()
    pl.semaphore_wait(barrier, 7)

    sends = []

    def start(make, *args):
        make(*args).start()
        sends.append((make, args))

    def raw_copy():
        return remote(tin.at[1 - c], rin, raw_sem.at[0], raw_sem.at[1], partner)

    start(raw_copy)
    for copy in w_loads[:2]:
        copy.wait()

    def weight_copy(n, i, role):
        size = WEIGHT_ROWS[n][1]
        mine, theirs = (n - 1, n + 3) if n else (3, 3)
        if role == 0:
            src, dst, at, to = mine, mine, (0, size), partner
        elif role == 1:
            src, dst, at, to = mine, theirs, (0, 0 if n else 2 * size), other
        else:
            src, dst, at, to = theirs, theirs, (0, size) if n else (2 * size, 3 * size), partner
        return remote(
            wb.at[src, pl.ds(i * 128 + at[0], size)],
            wb.at[dst, pl.ds(i * 128 + at[1], size)],
            w_send.at[role, n, i],
            w_recv.at[role, n, i],
            to,
        )

    for i in range(2):
        start(weight_copy, 0, i, 1)
    for copy in small:
        copy.wait()
    for copy in w_loads[2:]:
        copy.wait()
    for n in range(4):
        for i in range(2):
            start(weight_copy, n, i, 0)

    raw_copy().wait_recv()
    mine = tin[c].astype(F32)
    theirs = rin[...].astype(F32)
    square = jnp.sum(mine * mine, axis=1, keepdims=True) + jnp.sum(theirs * theirs, axis=1, keepdims=True)
    scaling = lax.rsqrt(square / 2048.0 + EPSILON)
    gain_v[...] = gain_ref[...].astype(F32)
    for part, at in ((mine, c), (theirs, 1 - c)):
        for i in range(8):
            lanes = pl.ds(pl.multiple_of(at * 1024 + 128 * i, 128), 128)
            gain = gain_v[pl.ds(8 * at + i, 1), :]
            tok[0, pl.ds(0, 64), lanes] = (part[:, 128 * i : 128 * i + 128] * scaling * gain).astype(BF16)

    def block(g, l, s, h):
        i, j = PLACE[l, s]
        return tok.at[4 * g + i, pl.ds(64 * j, 64 if g == 0 else ROW_A), pl.ds(1024 * h, 1024)]

    def token_copy(g, src, dst, h, to):
        return remote(
            block(g, *src, h), block(g, *dst, h), tok_send.at[g, *dst, h], tok_recv.at[g, *dst, h], to
        )

    def along_second(g, l, h):
        start(token_copy, g, (l, 0), (l, 1), h, s_next)
        start(token_copy, g, (l, 0), (l, 2), h, s_prev)

    def along_first(g, h, up):
        if up:
            start(token_copy, g, (0, 0), (1, 0), h, f_next)
        else:
            start(token_copy, g, (0, 0), (2, 0), h, f_prev)

    def edge(g, l, s):
        i, j = PLACE[l, s]
        return tok.at[4 * g + i, pl.ds(64 * j + ROW_A, 64 - ROW_A)]

    def edge_copy(l, s):
        return remote(edge(0, l, s), edge(1, l, s), b_send.at[l, s], b_recv.at[l, s], twin)

    def twin_copy(h):
        src = tok.at[0, pl.ds(0, ROW_A), pl.ds(1024 * h, 1024)]
        return remote(src, block(1, 0, 0, h), tok_send.at[1, 0, 0, h], tok_recv.at[1, 0, 0, h], twin)

    for h in range(2):
        along_first(0, h, True)
        along_first(0, 1 - h, False)
        start(twin_copy, h)
        start(token_copy, 0, (0, 0), (0, 1), h, s_next)
        start(token_copy, 0, (0, 0), (0, 2), 1 - h, s_prev)
    start(edge_copy, 0, 0)

    for copy in d_loads:
        copy.wait()
    folded[0] = jnp.dot(down_v[...], head_v[...], preferred_element_type=F32).astype(BF16)

    def head_copy(role):
        src, dst, to = ((0, 1, partner), (0, 2, other), (2, 3, partner))[role]
        return remote(folded.at[src], folded.at[dst], d_send.at[role], d_recv.at[role], to)

    start(head_copy, 1)
    start(head_copy, 0)
    for n in range(1, 4):
        for i in range(2):
            start(weight_copy, n, i, 1)

    def happen(event):
        kind = event[0]
        if kind == "r":
            _, g, l, s, h = event
            token_copy(g, (l, s), (l, s), h, partner).wait_recv()
            if s == 0:
                if l == 0:
                    along_first(g, h, True)
                    along_first(g, h, False)
                if (l, h) == (1, 0):
                    start(token_copy, g, (1, 0), (3, 0), 0, f_next)
                if (l, h) == (2, 1):
                    start(token_copy, g, (2, 0), (3, 0), 1, f_prev)
        elif kind == "q":
            along_second(*event[1:])
        elif kind == "f":
            _, g, l, h = event
            start(token_copy, g, (l, 1 + h), (l, 3), h, s_prev if h else s_next)
        elif kind == "e":
            start(edge_copy, event[1], event[2])
        elif kind == "B":
            edge_copy(event[1], event[2]).wait_recv()
        elif kind == "w":
            if event[1] == "d":
                head_copy(1).wait_recv()
                start(head_copy, 2)
            else:
                for i in range(2):
                    weight_copy(event[1], i, 1).wait_recv()
                    start(weight_copy, event[1], i, 2)
        elif event[1] != "d":
            for i in range(2):
                weight_copy(event[1], i, 2).wait_recv()
        else:
            head_copy(0).wait_recv()
            head_copy(2).wait_recv()
            for n in range(4):
                at, size = WEIGHT_ROWS[n]
                for j in range(4):
                    if n == 0:
                        heads[3, pl.ds(32 * j, 32)] = folded[j, pl.ds(at, size)]
                    else:
                        heads[n - 1 + 4 * (j // 2), pl.ds(64 * (j % 2), 64)] = folded[j, pl.ds(at, size)]

    for n in range(4):
        for i in range(2):
            weight_copy(n, i, 0).wait_recv()

    def gated(product, count):
        hidden = [
            (silu(product[:, 256 * k : 256 * k + 128]) * product[:, 256 * k + 128 : 256 * k + 256]).astype(BF16)
            for k in range(count)
        ]
        return jnp.concatenate(hidden, axis=1) if count > 1 else hidden[0]

    def unit(b, size, low, high):
        if high is None:
            count, weights, head = 1, wb[low], heads[low]
        else:
            count = high - low
            weights = wb[low:high].reshape(256 * count, 2048)
            head = heads[low:high].reshape(128 * count, 128)
        product = rows_by(tok[pl.ds(size * b, size)].reshape(256 * size, 2048), weights)
        value = jnp.dot(gated(product, count), head, preferred_element_type=F32)
        rows = pl.ds(pl.multiple_of(256 * size * b, 256), 256 * size)
        if high is not None and low == 0:
            acc[rows] = value
        else:
            acc[rows] += value

    def part_copy(g, l, s):
        to = device(x_two if g else x, (first + OFFSET[l]) % 4, (second + OFFSET[s]) % 4)
        i, j = PLACE[l, s]
        slot = 16 * g + 4 * SEEN_AS[l] + SEEN_AS[s]
        return remote(
            stage.at[4 * g + i, pl.ds(64 * j, 64)], parts.at[slot], rs_send.at[slot], rs_recv.at[slot], to
        )

    def finish(p, product):
        rows = pl.ds(512 * p, 512)
        total = acc[rows] + jnp.dot(gated(product, 1), heads[6], preferred_element_type=F32)
        stage[pl.ds(2 * p, 2)] = total.astype(BF16).reshape(2, 256, 128)
        for i in (2 * p + 1, 2 * p):
            for l, s in BLOCKS[i % 4]:
                if (i // 4, l, s) != (0, 0, 0):
                    part_copy(i // 4, l, s).start()
        if p == 0:
            acc[0:64] = total[0:64]

    def step(u, _):
        for i, (events, _) in enumerate(ORDER[:-1]):
            if events:

                @pl.when(u == i)
                def _():
                    for event in events:
                        happen(event)

        kind = pick(u, ["ABCDHIEFG".index(work[0]) for _, work in ORDER[:-1]])
        b = pick(u, [work[1] for _, work in ORDER[:-1]])
        for i, (low, high) in enumerate(((0, 4), (0, 5), (0, 6), (4, 6), (5, 6), (4, 5))):

            @pl.when(kind == i)
            def _():
                unit(b, 1, low, high)

        @pl.when((kind == 6) | (kind == 7))
        def _():
            unit(b, 2, kind - 2, None)

        return 0

    lax.fori_loop(0, len(ORDER) - 1, step, 0)

    for event in ORDER[-1][0]:
        happen(event)
    product = None
    for p in (3, 2, 1, 0):
        ahead = rows_by(tok[2 * p : 2 * p + 2].reshape(512, 2048), wb[6])
        if p < 3:
            finish(p + 1, product)
        product = ahead
    finish(0, product)

    spot = lax.broadcasted_iota(jnp.int32, (64, 128), 1) == lax.broadcasted_iota(jnp.int32, (64, 128), 0) + 64 * c

    def upright(ref, i):
        return jnp.sum(jnp.where(spot, ref[i : i + 1, :], 0), axis=1, keepdims=True)

    ids = [upright(ids_ref, i) for i in range(2)]
    codes = [upright(codes_ref, i).astype(F32) for i in range(2)]
    share = [code / (codes[0] + codes[1]) for code in codes]
    shares = []
    for j in range(4):
        e = (z + OFFSET[j]) % 4
        shares.append(jnp.where(ids[0] == e, share[0], 0.0) + jnp.where(ids[1] == e, share[1], 0.0))
    c_wide = c.astype(F32)

    def arrived(slot):
        remote(parts.at[slot], parts.at[slot], rs_send.at[slot], rs_recv.at[slot], partner).wait_recv()
        return parts[slot].astype(F32)

    blended = jnp.zeros((64, 128), F32)
    for s in (3, 2, 1, 0):
        for l in (3, 2, 1, 0):
            slot = 4 * l + s
            weight = shares[s] * (1.0 - c_wide) + shares[l] * c_wide
            far = arrived(16 + slot)
            near = arrived(slot) if slot else acc[0:64]
            blended += (near + far) * weight
    rows = pl.ds(pl.multiple_of(64 * c, 64), 64)
    final_ref[rows] = blended

    def final_copy():
        return remote(final_ref.at[rows], final_ref.at[rows], fin_sem.at[0], fin_sem.at[1], partner)

    start(final_copy)
    final_copy().wait_recv()

    for make, args in sends:
        make(*args).wait_send()
    for slot in range(1, 32):
        remote(parts.at[slot], parts.at[slot], rs_send.at[slot], rs_recv.at[slot], partner).wait_send()


def last_kernel(final_ref, actions_ref, rewards_ref, trace_ref, values_ref, targets_ref):
    values = final_ref[...]
    values_ref[...] = values
    lane = lax.broadcasted_iota(jnp.int32, (128, 128), 1)
    row = lax.broadcasted_iota(jnp.int32, (128, 128), 0)

    def column(v):
        return jnp.sum(jnp.where(lane == row, v, 0.0), axis=1, keepdims=True)

    trace = trace_ref[...].astype(F32) / 1024.0
    reward = rewards_ref[...].astype(F32) * 0.25
    action_column = jnp.sum(jnp.where(lane == row, actions_ref[...], 0), axis=1, keepdims=True)
    greedy = jnp.max(values, axis=1, keepdims=True)
    taken = jnp.sum(jnp.where(lane == action_column, values, 0.0), axis=1, keepdims=True)
    ahead = greedy - column(trace) * taken
    driver = reward + DISCOUNT * jnp.sum(jnp.where(row == lane + 1, ahead, 0.0), axis=0, keepdims=True)
    logs = jnp.log(DISCOUNT * trace)
    sums_column = jnp.sum(jnp.where(lane <= row, logs, 0.0), axis=1, keepdims=True)
    sums_row = jnp.sum(jnp.where(lane == row, sums_column, 0.0), axis=0, keepdims=True)
    weight = jnp.where(lane >= row, jnp.exp(jnp.minimum(sums_row - sums_column, 0.0)), 0.0)
    target = jnp.sum(weight * driver, axis=1, keepdims=True)
    targets_ref[...] = jnp.sum(jnp.where(lane == row, target, 0.0), axis=0, keepdims=True)


def per_device(
    tokens,
    norm_gain,
    expert_ids,
    gate_codes,
    gate_weights,
    up_weights,
    down_weights,
    value_head,
    actions,
    rewards,
    trace_codes,
):
    dma = pltpu.SemaphoreType.DMA
    vmem, hbm = pl.BlockSpec(memory_space=pltpu.VMEM), pl.BlockSpec(memory_space=pl.ANY)
    final = pl.pallas_call(
        kernel,
        out_shape=pltpu.VMEM((128, 128), F32),
        in_specs=[hbm] * 8,
        out_specs=vmem,
        scratch_shapes=[
            pltpu.VMEM((16, 128), BF16),
            pltpu.VMEM((2, 128), jnp.int32),
            pltpu.VMEM((2, 128), jnp.int32),
            pltpu.VMEM((2, 64, 1024), BF16),
            pltpu.VMEM((64, 1024), BF16),
            pltpu.VMEM((8, 256, 2048), BF16),
            pltpu.VMEM((7, 256, 2048), BF16),
            pltpu.VMEM((224, 2048), BF16),
            pltpu.VMEM((2048, 128), BF16),
            pltpu.VMEM((4, 224, 128), BF16),
            pltpu.VMEM((7, 128, 128), BF16),
            pltpu.VMEM((2048, 128), F32),
            pltpu.VMEM((8, 256, 128), BF16),
            pltpu.VMEM((32, 64, 128), BF16),
            pltpu.VMEM((16, 128), F32),
            dma((15,)),
            dma((2,)),
            dma((2, 4, 4, 2)),
            dma((2, 4, 4, 2)),
            dma((4, 4)),
            dma((4, 4)),
            dma((3, 4, 2)),
            dma((3, 4, 2)),
            dma((3,)),
            dma((3,)),
            dma((32,)),
            dma((32,)),
            dma((2,)),
        ],
        compiler_params=pltpu.CompilerParams(
            collective_id=0, has_side_effects=True, vmem_limit_bytes=56 * 1024 * 1024
        ),
        name="critic",
    )(
        tokens,
        norm_gain.reshape(16, 128),
        expert_ids.T,
        gate_codes.T,
        gate_weights,
        up_weights,
        down_weights,
        value_head,
    )
    values, targets = pl.pallas_call(
        last_kernel,
        out_shape=(jax.ShapeDtypeStruct((128, 128), F32), jax.ShapeDtypeStruct((1, 128), F32)),
        in_specs=[vmem] * 4,
        out_specs=(vmem, vmem),
        name="retrace",
    )(pltpu.with_memory_space_constraint(final, pltpu.VMEM), actions.reshape(1, -1), rewards.reshape(1, -1), trace_codes.reshape(1, -1))
    return values, targets.reshape(-1)


def solution(mesh):
    group, weight = P(("dp", "expert"), None), P("expert", ("dp", "tensor"), None)
    line = P(("dp", "expert"))
    in_specs = (
        P(("dp", "expert"), "tensor"),
        P(),
        group,
        group,
        weight,
        weight,
        weight,
        P(),
        line,
        line,
        line,
    )
    return jax.shard_map(
        per_device, mesh=mesh, in_specs=in_specs, out_specs=(group, line), check_vma=False
    )
```

```python
import functools

import jax
import jax.numpy as jnp
from jax import lax
from jax.experimental import pallas as pl
from jax.experimental.pallas import tpu as pltpu
from jax.sharding import PartitionSpec as P

DISCOUNT = 0.99
EPSILON = 1e-05
MESH = pl.DeviceIdType.MESH
F32, BF16 = jnp.float32, jnp.bfloat16

OFFSET = (0, 3, 1, 2)
SEEN_AS = (0, 2, 1, 3)
ROW_A = 48
WEIGHT_ROWS = ((0, 32), (32, 64), (96, 64), (160, 64))


def rows_by(a, b):
    return lax.dot_general(a, b, (((1,), (1,)), ((), ())), preferred_element_type=F32)


def silu(v):
    return v / (1.0 + jnp.exp(-v))


ORDER = (
    (
        (
            ("r", 1, 0, 0, 0), ("q", 1, 0, 0), ("w", 0), ("r", 0, 1, 0, 0), ("q", 0, 1, 0), ("r", 0, 2, 0, 1),
            ("q", 0, 2, 1), ("r", 0, 0, 1, 0), ("r", 0, 0, 2, 1), ("w", "d"), ("r", 1, 0, 0, 1), ("p", 0),
            ("f", 0, 0, 0), ("f", 0, 0, 1), ("p", "d"), ("r", 0, 1, 0, 1), ("e", 1, 0), ("r", 0, 2, 0, 0),
            ("e", 2, 0), ("r", 0, 0, 1, 1), ("e", 0, 1), ("r", 0, 0, 2, 0), ("e", 0, 2), ("B", 0, 0),
            ("q", 0, 1, 1), ("r", 1, 1, 0, 0), ("r", 1, 2, 0, 0), ("r", 1, 0, 1, 0), ("r", 1, 0, 2, 0),
            ("q", 0, 2, 0), ("B", 1, 0), ("r", 0, 3, 0, 0), ("r", 0, 3, 0, 1), ("e", 3, 0), ("r", 0, 1, 1, 0),
            ("r", 0, 1, 2, 0),
        ),
        ("A", 0),
    ),
    (
        (
            ("B", 2, 0), ("f", 0, 1, 0), ("r", 1, 1, 0, 1), ("r", 1, 2, 0, 1), ("r", 0, 2, 2, 1),
            ("f", 0, 2, 1), ("B", 0, 1), ("r", 0, 2, 1, 1), ("q", 0, 3, 0), ("r", 0, 0, 3, 1), ("B", 0, 2),
            ("r", 1, 3, 0, 0), ("q", 0, 3, 1), ("w", 1), ("r", 0, 0, 3, 0), ("e", 0, 3), ("r", 0, 1, 2, 1),
            ("e", 1, 2), ("B", 3, 0), ("f", 0, 1, 1), ("f", 1, 0, 0), ("r", 0, 1, 1, 1), ("e", 1, 1),
        ),
        ("A", 1),
    ),
    (
        (
            ("q", 1, 0, 1), ("p", 1), ("r", 1, 3, 0, 1), ("r", 0, 2, 1, 0), ("e", 2, 1), ("r", 0, 2, 2, 0),
            ("e", 2, 2),
        ),
        ("B", 4),
    ),
    (
        (
            ("f", 0, 2, 0), ("q", 1, 1, 0), ("r", 0, 1, 3, 0), ("r", 0, 2, 3, 1), ("B", 0, 3),
        ),
        ("E", 0),
    ),
    (
        (
            ("q", 1, 1, 1), ("r", 0, 3, 1, 0), ("r", 0, 3, 2, 0), ("B", 1, 2), ("f", 0, 3, 0),
            ("r", 0, 3, 1, 1), ("e", 3, 1), ("r", 0, 3, 2, 1), ("e", 3, 2), ("f", 0, 3, 1),
        ),
        ("B", 2),
    ),
    (
        (
            ("q", 1, 2, 0), ("B", 1, 1), ("r", 1, 0, 3, 0), ("r", 0, 1, 3, 1), ("e", 1, 3), ("B", 2, 1),
            ("q", 1, 2, 1), ("r", 1, 0, 1, 1), ("r", 1, 0, 2, 1), ("f", 1, 0, 1), ("q", 1, 3, 0), ("B", 2, 2),
            ("r", 0, 2, 3, 0), ("e", 2, 3), ("r", 1, 1, 2, 0), ("w", 2), ("q", 1, 3, 1), ("r", 1, 1, 1, 0),
            ("r", 1, 1, 2, 1), ("B", 3, 1), ("f", 1, 1, 0), ("f", 1, 1, 1), ("r", 1, 1, 1, 1),
        ),
        ("B", 5),
    ),
    (
        (
            ("p", 2), ("r", 0, 3, 3, 1), ("B", 3, 2), ("r", 0, 3, 3, 0), ("e", 3, 3), ("r", 1, 2, 2, 0),
            ("B", 1, 3),
        ),
        ("C", 3),
    ),
    (
        (
            ("r", 1, 2, 1, 0), ("f", 1, 2, 0), ("r", 1, 2, 2, 1), ("f", 1, 2, 1), ("B", 2, 3),
            ("r", 1, 2, 1, 1), ("r", 1, 0, 3, 1),
        ),
        ("F", 0),
    ),
    (
        (
            ("r", 1, 3, 1, 0), ("f", 1, 3, 0), ("r", 1, 3, 2, 0),
        ),
        ("F", 2),
    ),
    (
        (
            ("r", 1, 3, 1, 1), ("r", 1, 3, 2, 1), ("f", 1, 3, 1),
        ),
        ("C", 6),
    ),
    (
        (
            ("B", 3, 3), ("r", 1, 1, 3, 0), ("r", 1, 1, 3, 1), ("r", 1, 2, 3, 0), ("r", 1, 2, 3, 1),
        ),
        ("H", 2),
    ),
    (
        (
            ("w", 3), ("r", 1, 3, 3, 0), ("r", 1, 3, 3, 1),
        ),
        ("C", 7),
    ),
    (
        (
            ("p", 3),
        ),
        ("G", 0),
    ),
)

BLOCKS = (
    ((0, 0), (1, 0), (2, 0), (3, 0)),
    ((0, 1), (0, 2), (1, 1), (1, 2)),
    ((2, 1), (2, 2), (3, 1), (3, 2)),
    ((0, 3), (1, 3), (2, 3), (3, 3)),
)
PLACE = {block: (i, j) for i, blocks in enumerate(BLOCKS) for j, block in enumerate(blocks)}


def pick(index, values):
    out = values[-1]
    for i in range(len(values) - 2, -1, -1):
        out = jnp.where(index == i, values[i], out)
    return out


def kernel(
    tokens_ref,
    gain_hbm,
    ids_hbm,
    codes_hbm,
    gate_ref,
    up_ref,
    down_ref,
    head_ref,
    final_ref,
    gain_ref,
    ids_ref,
    codes_ref,
    tin,
    rin,
    tok,
    wb,
    down_v,
    head_v,
    folded,
    heads,
    acc,
    stage,
    parts,
    gain_v,
    local_sem,
    raw_sem,
    tok_recv,
    tok_send,
    b_recv,
    b_send,
    w_recv,
    w_send,
    d_recv,
    d_send,
    rs_recv,
    rs_send,
    fin_sem,
):
    dp, z, c = lax.axis_index("dp"), lax.axis_index("expert"), lax.axis_index("tensor")
    x, y = dp % 4, dp // 4
    x_one = x + 1 - 2 * (x % 2)
    x_two = (x + 2 * (x % 2) + 3) % 4
    first, second = y * (1 - c) + z * c, z * (1 - c) + y * c

    def device(x_, f_, s_):
        y_, z_ = f_ * (1 - c) + s_ * c, s_ * (1 - c) + f_ * c
        return (y_ * 4 + x_, z_, c)

    partner = (dp, z, 1 - c)
    other = (y * 4 + x_one, z, c)
    twin = device(x_two, first, second)
    f_next = device(x, (first + 1) % 4, second)
    f_prev = device(x, (first + 3) % 4, second)
    s_next = device(x, first, (second + 1) % 4)
    s_prev = device(x, first, (second + 3) % 4)

    def remote(src, dst, send, recv, to):
        return pltpu.make_async_remote_copy(
            src_ref=src, dst_ref=dst, send_sem=send, recv_sem=recv, device_id=to, device_id_type=MESH
        )

    barrier = pltpu.get_barrier_semaphore()
    for to in (partner, other, twin, f_next, f_prev, s_next, s_prev):
        pl.semaphore_signal(barrier, inc=1, device_id=to, device_id_type=MESH)
    loads = [pltpu.make_async_copy(tokens_ref.at[pl.ds(i * 64, 64)], tin.at[i], local_sem.at[i]) for i in range(2)]
    w_loads = []
    for n, (at, size) in enumerate(WEIGHT_ROWS):
        chunk = n - 1 if n else 3
        for i, ref in enumerate((gate_ref, up_ref)):
            w_loads.append(
                pltpu.make_async_copy(
                    ref.at[0, pl.ds(at, size)], wb.at[chunk, pl.ds(i * 128, size)], local_sem.at[2 + 2 * n + i]
                )
            )
    d_loads = [
        pltpu.make_async_copy(down_ref.at[0], down_v, local_sem.at[10]),
        pltpu.make_async_copy(head_ref, head_v, local_sem.at[11]),
    ]
    small = [
        pltpu.make_async_copy(src, dst, local_sem.at[12 + i])
        for i, (src, dst) in enumerate(((gain_hbm, gain_ref), (ids_hbm, ids_ref), (codes_hbm, codes_ref)))
    ]
    for copy in loads + w_loads[:2] + small[:1] + w_loads[2:] + d_loads + small[1:]:
        copy.start()

    for copy in loads:
        copy.wait()
    pl.semaphore_wait(barrier, 7)

    sends = []

    def start(make, *args):
        make(*args).start()
        sends.append((make, args))

    def raw_copy():
        return remote(tin.at[1 - c], rin, raw_sem.at[0], raw_sem.at[1], partner)

    start(raw_copy)
    for copy in w_loads[:2]:
        copy.wait()

    def weight_copy(n, i, role):
        size = WEIGHT_ROWS[n][1]
        mine, theirs = (n - 1, n + 3) if n else (3, 3)
        if role == 0:
            src, dst, at, to = mine, mine, (0, size), partner
        elif role == 1:
            src, dst, at, to = mine, theirs, (0, 0 if n else 2 * size), other
        else:
            src, dst, at, to = theirs, theirs, (0, size) if n else (2 * size, 3 * size), partner
        return remote(
            wb.at[src, pl.ds(i * 128 + at[0], size)],
            wb.at[dst, pl.ds(i * 128 + at[1], size)],
            w_send.at[role, n, i],
            w_recv.at[role, n, i],
            to,
        )

    for i in range(2):
        start(weight_copy, 0, i, 1)
    for copy in small:
        copy.wait()
    for copy in w_loads[2:]:
        copy.wait()
    for n in range(4):
        for i in range(2):
            start(weight_copy, n, i, 0)

    raw_copy().wait_recv()
    mine = tin[c].astype(F32)
    theirs = rin[...].astype(F32)
    square = jnp.sum(mine * mine, axis=1, keepdims=True) + jnp.sum(theirs * theirs, axis=1, keepdims=True)
    scaling = lax.rsqrt(square / 2048.0 + EPSILON)
    gain_v[...] = gain_ref[...].astype(F32)
    for part, at in ((mine, c), (theirs, 1 - c)):
        for i in range(8):
            lanes = pl.ds(pl.multiple_of(at * 1024 + 128 * i, 128), 128)
            gain = gain_v[pl.ds(8 * at + i, 1), :]
            tok[0, pl.ds(0, 64), lanes] = (part[:, 128 * i : 128 * i + 128] * scaling * gain).astype(BF16)

    def block(g, l, s, h):
        i, j = PLACE[l, s]
        return tok.at[4 * g + i, pl.ds(64 * j, 64 if g == 0 else ROW_A), pl.ds(1024 * h, 1024)]

    def token_copy(g, src, dst, h, to):
        return remote(
            block(g, *src, h), block(g, *dst, h), tok_send.at[g, *dst, h], tok_recv.at[g, *dst, h], to
        )

    def along_second(g, l, h):
        start(token_copy, g, (l, 0), (l, 1), h, s_next)
        start(token_copy, g, (l, 0), (l, 2), h, s_prev)

    def along_first(g, h, up):
        if up:
            start(token_copy, g, (0, 0), (1, 0), h, f_next)
        else:
            start(token_copy, g, (0, 0), (2, 0), h, f_prev)

    def edge(g, l, s):
        i, j = PLACE[l, s]
        return tok.at[4 * g + i, pl.ds(64 * j + ROW_A, 64 - ROW_A)]

    def edge_copy(l, s):
        return remote(edge(0, l, s), edge(1, l, s), b_send.at[l, s], b_recv.at[l, s], twin)

    def twin_copy(h):
        src = tok.at[0, pl.ds(0, ROW_A), pl.ds(1024 * h, 1024)]
        return remote(src, block(1, 0, 0, h), tok_send.at[1, 0, 0, h], tok_recv.at[1, 0, 0, h], twin)

    for h in range(2):
        along_first(0, h, True)
        along_first(0, 1 - h, False)
        start(twin_copy, h)
        start(token_copy, 0, (0, 0), (0, 1), h, s_next)
        start(token_copy, 0, (0, 0), (0, 2), 1 - h, s_prev)
    start(edge_copy, 0, 0)

    for copy in d_loads:
        copy.wait()
    folded[0] = jnp.dot(down_v[...], head_v[...], preferred_element_type=F32).astype(BF16)

    def head_copy(role):
        src, dst, to = ((0, 1, partner), (0, 2, other), (2, 3, partner))[role]
        return remote(folded.at[src], folded.at[dst], d_send.at[role], d_recv.at[role], to)

    start(head_copy, 1)
    start(head_copy, 0)
    for n in range(1, 4):
        for i in range(2):
            start(weight_copy, n, i, 1)

    def happen(event):
        kind = event[0]
        if kind == "r":
            _, g, l, s, h = event
            token_copy(g, (l, s), (l, s), h, partner).wait_recv()
            if s == 0:
                if l == 0:
                    along_first(g, h, True)
                    along_first(g, h, False)
                if (l, h) == (1, 0):
                    start(token_copy, g, (1, 0), (3, 0), 0, f_next)
                if (l, h) == (2, 1):
                    start(token_copy, g, (2, 0), (3, 0), 1, f_prev)
        elif kind == "q":
            along_second(*event[1:])
        elif kind == "f":
            _, g, l, h = event
            start(token_copy, g, (l, 1 + h), (l, 3), h, s_prev if h else s_next)
        elif kind == "e":
            start(edge_copy, event[1], event[2])
        elif kind == "B":
            edge_copy(event[1], event[2]).wait_recv()
        elif kind == "w":
            if event[1] == "d":
                head_copy(1).wait_recv()
                start(head_copy, 2)
            else:
                for i in range(2):
                    weight_copy(event[1], i, 1).wait_recv()
                    start(weight_copy, event[1], i, 2)
        elif event[1] != "d":
            for i in range(2):
                weight_copy(event[1], i, 2).wait_recv()
        else:
            head_copy(0).wait_recv()
            head_copy(2).wait_recv()
            for n in range(4):
                at, size = WEIGHT_ROWS[n]
                for j in range(4):
                    if n == 0:
                        heads[3, pl.ds(32 * j, 32)] = folded[j, pl.ds(at, size)]
                    else:
                        heads[n - 1 + 4 * (j // 2), pl.ds(64 * (j % 2), 64)] = folded[j, pl.ds(at, size)]

    for n in range(4):
        for i in range(2):
            weight_copy(n, i, 0).wait_recv()

    def gated(product, count):
        hidden = [
            (silu(product[:, 256 * k : 256 * k + 128]) * product[:, 256 * k + 128 : 256 * k + 256]).astype(BF16)
            for k in range(count)
        ]
        return jnp.concatenate(hidden, axis=1) if count > 1 else hidden[0]

    def unit(b, size, low, high):
        if high is None:
            count, weights, head = 1, wb[low], heads[low]
        else:
            count = high - low
            weights = wb[low:high].reshape(256 * count, 2048)
            head = heads[low:high].reshape(128 * count, 128)
        product = rows_by(tok[pl.ds(size * b, size)].reshape(256 * size, 2048), weights)
        value = jnp.dot(gated(product, count), head, preferred_element_type=F32)
        rows = pl.ds(pl.multiple_of(256 * size * b, 256), 256 * size)
        if high is not None and low == 0:
            acc[rows] = value
        else:
            acc[rows] += value

    def part_copy(g, l, s):
        to = device(x_two if g else x, (first + OFFSET[l]) % 4, (second + OFFSET[s]) % 4)
        i, j = PLACE[l, s]
        slot = 16 * g + 4 * SEEN_AS[l] + SEEN_AS[s]
        return remote(
            stage.at[4 * g + i, pl.ds(64 * j, 64)], parts.at[slot], rs_send.at[slot], rs_recv.at[slot], to
        )

    def finish(p, product):
        rows = pl.ds(512 * p, 512)
        total = acc[rows] + jnp.dot(gated(product, 1), heads[6], preferred_element_type=F32)
        stage[pl.ds(2 * p, 2)] = total.astype(BF16).reshape(2, 256, 128)
        for i in (2 * p + 1, 2 * p):
            for l, s in BLOCKS[i % 4]:
                if (i // 4, l, s) != (0, 0, 0):
                    part_copy(i // 4, l, s).start()
        if p == 0:
            acc[0:64] = total[0:64]

    def step(u, _):
        for i, (events, _) in enumerate(ORDER[:-1]):
            if events:

                @pl.when(u == i)
                def _():
                    for event in events:
                        happen(event)

        kind = pick(u, ["ABCDHIEFG".index(work[0]) for _, work in ORDER[:-1]])
        b = pick(u, [work[1] for _, work in ORDER[:-1]])
        for i, (low, high) in enumerate(((0, 4), (0, 5), (0, 6), (4, 6), (5, 6), (4, 5))):

            @pl.when(kind == i)
            def _():
                unit(b, 1, low, high)

        @pl.when((kind == 6) | (kind == 7))
        def _():
            unit(b, 2, kind - 2, None)

        return 0

    lax.fori_loop(0, len(ORDER) - 1, step, 0)

    for event in ORDER[-1][0]:
        happen(event)
    product = None
    for p in (3, 2, 1, 0):
        ahead = rows_by(tok[2 * p : 2 * p + 2].reshape(512, 2048), wb[6])
        if p < 3:
            finish(p + 1, product)
        product = ahead
    finish(0, product)

    spot = lax.broadcasted_iota(jnp.int32, (64, 128), 1) == lax.broadcasted_iota(jnp.int32, (64, 128), 0) + 64 * c

    def upright(ref, i):
        return jnp.sum(jnp.where(spot, ref[i : i + 1, :], 0), axis=1, keepdims=True)

    ids = [upright(ids_ref, i) for i in range(2)]
    codes = [upright(codes_ref, i).astype(F32) for i in range(2)]
    share = [code / (codes[0] + codes[1]) for code in codes]
    shares = []
    for j in range(4):
        e = (z + OFFSET[j]) % 4
        shares.append(jnp.where(ids[0] == e, share[0], 0.0) + jnp.where(ids[1] == e, share[1], 0.0))
    c_wide = c.astype(F32)

    def arrived(slot):
        remote(parts.at[slot], parts.at[slot], rs_send.at[slot], rs_recv.at[slot], partner).wait_recv()
        return parts[slot].astype(F32)

    for make, args in sends:
        make(*args).wait_send()
    blended = jnp.zeros((64, 128), F32)
    for s in (3, 2, 1, 0):
        for l in (3, 2, 1, 0):
            slot = 4 * l + s
            weight = shares[s] * (1.0 - c_wide) + shares[l] * c_wide
            far = arrived(16 + slot)
            near = arrived(slot) if slot else acc[0:64]
            blended += (near + far) * weight
    rows = pl.ds(pl.multiple_of(64 * c, 64), 64)
    final_ref[rows] = blended

    def final_copy():
        return remote(final_ref.at[rows], final_ref.at[rows], fin_sem.at[0], fin_sem.at[1], partner)

    final_copy().start()
    for slot in range(1, 32):
        remote(parts.at[slot], parts.at[slot], rs_send.at[slot], rs_recv.at[slot], partner).wait_send()
    final_copy().wait_recv()
    final_copy().wait_send()


def last_kernel(final_ref, actions_ref, rewards_ref, trace_ref, values_ref, targets_ref):
    values = final_ref[...]
    values_ref[...] = values
    lane = lax.broadcasted_iota(jnp.int32, (128, 128), 1)
    row = lax.broadcasted_iota(jnp.int32, (128, 128), 0)

    def column(v):
        return jnp.sum(jnp.where(lane == row, v, 0.0), axis=1, keepdims=True)

    trace = trace_ref[...].astype(F32) / 1024.0
    reward = rewards_ref[...].astype(F32) * 0.25
    action_column = jnp.sum(jnp.where(lane == row, actions_ref[...], 0), axis=1, keepdims=True)
    greedy = jnp.max(values, axis=1, keepdims=True)
    taken = jnp.sum(jnp.where(lane == action_column, values, 0.0), axis=1, keepdims=True)
    ahead = greedy - column(trace) * taken
    driver = reward + DISCOUNT * jnp.sum(jnp.where(row == lane + 1, ahead, 0.0), axis=0, keepdims=True)
    logs = jnp.log(DISCOUNT * trace)
    sums_column = jnp.sum(jnp.where(lane <= row, logs, 0.0), axis=1, keepdims=True)
    sums_row = jnp.sum(jnp.where(lane == row, sums_column, 0.0), axis=0, keepdims=True)
    weight = jnp.where(lane >= row, jnp.exp(jnp.minimum(sums_row - sums_column, 0.0)), 0.0)
    target = jnp.sum(weight * driver, axis=1, keepdims=True)
    targets_ref[...] = jnp.sum(jnp.where(lane == row, target, 0.0), axis=0, keepdims=True)


def per_device(
    tokens,
    norm_gain,
    expert_ids,
    gate_codes,
    gate_weights,
    up_weights,
    down_weights,
    value_head,
    actions,
    rewards,
    trace_codes,
):
    dma = pltpu.SemaphoreType.DMA
    vmem, hbm = pl.BlockSpec(memory_space=pltpu.VMEM), pl.BlockSpec(memory_space=pl.ANY)
    final = pl.pallas_call(
        kernel,
        out_shape=pltpu.VMEM((128, 128), F32),
        in_specs=[hbm] * 8,
        out_specs=vmem,
        scratch_shapes=[
            pltpu.VMEM((16, 128), BF16),
            pltpu.VMEM((2, 128), jnp.int32),
            pltpu.VMEM((2, 128), jnp.int32),
            pltpu.VMEM((2, 64, 1024), BF16),
            pltpu.VMEM((64, 1024), BF16),
            pltpu.VMEM((8, 256, 2048), BF16),
            pltpu.VMEM((7, 256, 2048), BF16),
            pltpu.VMEM((224, 2048), BF16),
            pltpu.VMEM((2048, 128), BF16),
            pltpu.VMEM((4, 224, 128), BF16),
            pltpu.VMEM((7, 128, 128), BF16),
            pltpu.VMEM((2048, 128), F32),
            pltpu.VMEM((8, 256, 128), BF16),
            pltpu.VMEM((32, 64, 128), BF16),
            pltpu.VMEM((16, 128), F32),
            dma((15,)),
            dma((2,)),
            dma((2, 4, 4, 2)),
            dma((2, 4, 4, 2)),
            dma((4, 4)),
            dma((4, 4)),
            dma((3, 4, 2)),
            dma((3, 4, 2)),
            dma((3,)),
            dma((3,)),
            dma((32,)),
            dma((32,)),
            dma((2,)),
        ],
        compiler_params=pltpu.CompilerParams(
            collective_id=0, has_side_effects=True, vmem_limit_bytes=56 * 1024 * 1024
        ),
        name="critic",
    )(
        tokens,
        norm_gain.reshape(16, 128),
        expert_ids.T,
        gate_codes.T,
        gate_weights,
        up_weights,
        down_weights,
        value_head,
    )
    values, targets = pl.pallas_call(
        last_kernel,
        out_shape=(jax.ShapeDtypeStruct((128, 128), F32), jax.ShapeDtypeStruct((1, 128), F32)),
        in_specs=[vmem] * 4,
        out_specs=(vmem, vmem),
        name="retrace",
    )(pltpu.with_memory_space_constraint(final, pltpu.VMEM), actions.reshape(1, -1), rewards.reshape(1, -1), trace_codes.reshape(1, -1))
    return values, targets.reshape(-1)


def solution(mesh):
    group, weight = P(("dp", "expert"), None), P("expert", ("dp", "tensor"), None)
    line = P(("dp", "expert"))
    in_specs = (
        P(("dp", "expert"), "tensor"),
        P(),
        group,
        group,
        weight,
        weight,
        weight,
        P(),
        line,
        line,
        line,
    )
    return jax.shard_map(
        per_device, mesh=mesh, in_specs=in_specs, out_specs=(group, line), check_vma=False
    )
```
